32 devices in a mesh: grp: 2 (over y), dom: 16 (over z, x, core).
Axes of the slice: x: 2, y: 2, z: 4, core: 2. Of those that a mesh axis runs over, the one named last changes fastest.
Arguments:
- user_table: float32 [32768, 256], P(('grp', 'dom')), may hold values from -96 to 96
- user_accum: float32 [32768, 256], P(('grp', 'dom')), may hold values from 0.05 to 1
- item_table: float32 [32768, 256], P(('grp', 'dom')), may hold values from -11 to 11
- item_accum: float32 [32768, 256], P(('grp', 'dom')), may hold values from 0.05 to 1
- block_pick: int32 [2, 2, 32], P(None, None, ('grp', 'dom')), may hold values from 0 to 7
- positives: int32 [2, 2, 16384], P(None, None, ('grp', 'dom')), may hold values from 0 to 255
- partners: int32 [2, 16], replicated, may hold values from 0 to 15, as said below
Outputs:
- users_out: float32 [32768, 256], P(('grp', 'dom'))
- user_accum_out: float32 [32768, 256], P(('grp', 'dom'))
- items_out: float32 [32768, 256], P(('grp', 'dom'))
- item_accum_out: float32 [32768, 256], P(('grp', 'dom'))
The draws below stay inside these ranges and needn't reach their ends.
Inputs may be any that keep to these rules, and one draw needn't show every extreme that they name: partners[b, d] equals d XOR 2**j_b for one whole number j_b of 0 to log2(16) - 1 in each bucket.
All inputs are finite; a program needn't handle non-finite values.
Results may differ from the reference program's by a relative error of at most 0.0008.
Values sent between devices are 32-bit elements; how exact they have to be, the bound alone decides.
A program may use at most 64 MiB of HBM per device.

```python
import math
import jax
import jax.numpy as jnp
from jax import lax

D = 256
BLOCK = 128
BUCKETS = 2
INNER = 2
USR_DEV = 1024
ITEM_DEV = 1024
USER_SPAN = 512
USERS = 32768
ITEMS = 32768
BATCH = 256
N_GRP = 2
N_DOM = 16
DEVICES = 32


def draw_user_table(key, part):
    sub_key = jax.random.fold_in(key, 1)
    return jnp.clip(0.5 * jax.random.normal(sub_key, (USERS, D), jnp.float32), -3.0, 3.0)


def draw_item_table(key, part):
    sub_key = jax.random.fold_in(key, 2)
    return jnp.clip(0.4 * jax.random.normal(sub_key, (ITEMS, D), jnp.float32), -2.4, 2.4)


def draw_partners(key, part):
    levels = N_DOM.bit_length() - 1
    level_pick = jax.random.randint(jax.random.fold_in(key, 3), (BUCKETS, 1), 0, levels, dtype=jnp.int32)
    masks = jnp.left_shift(jnp.ones_like(level_pick), level_pick)
    groups = jnp.arange(N_DOM, dtype=jnp.int32)[None, :]
    return jnp.bitwise_xor(groups, masks).astype(jnp.int32)


def set_ends(drawn, stream_key, least, largest):
    extent = drawn.shape
    index_at = [jax.random.randint(jax.random.fold_in(stream_key, axis), (), 0, extent[axis]) for axis in range(len(extent))]
    drawn = drawn.at[tuple(index_at)].set(least)
    longest = extent.index(max(extent))
    index_at[longest] = (index_at[longest] + 1) % extent[longest]
    return drawn.at[tuple(index_at)].set(largest)


def block_levels(stream_key, extent, cuts, least, largest):
    def one(dim, shards_of):
        heights = jax.random.uniform(jax.random.fold_in(jax.random.fold_in(stream_key, 6), dim), (shards_of,), jnp.float32, least / len(cuts), largest / len(cuts))
        return jnp.repeat(jnp.exp(heights), extent[dim] // shards_of).reshape((-1,) + (1,) * (len(extent) - dim - 1))

    level = one(*cuts[0])
    for cut in cuts[1:]:
        level = level * one(*cut)
    return level


def setup_inputs(seed: int = 0) -> dict:
    seeds = jax.random.split(jax.random.key(seed), 8)
    return {
        "user_table": draw_user_table(jax.random.fold_in(seeds[7], 71), 0),
        "user_accum": jnp.clip(jnp.exp(math.log(1.0) - 2.9957323 * jax.random.uniform(seeds[1], (USERS, D), jnp.float32) ** block_levels(seeds[1], (USERS, D), ((0, 32),), -0.2, 0.2)), 0.05, 1.0),
        "item_table": draw_item_table(jax.random.fold_in(seeds[7], 71), 0),
        "item_accum": jnp.clip(jnp.exp(math.log(1.0) - 2.9957323 * jax.random.uniform(seeds[3], (ITEMS, D), jnp.float32) ** block_levels(seeds[3], (ITEMS, D), ((0, 32),), -0.2, 0.2)), 0.05, 1.0),
        "block_pick": set_ends(jax.random.randint(seeds[4], (BUCKETS, INNER, DEVICES), 0, ITEM_DEV // BLOCK), jax.random.fold_in(seeds[4], 1), 0, (ITEM_DEV // BLOCK) - 1).astype(jnp.int32),
        "positives": set_ends(jax.random.randint(seeds[5], (BUCKETS, INNER, USER_SPAN * DEVICES), 0, BATCH), jax.random.fold_in(seeds[5], 1), 0, BATCH - 1).astype(jnp.int32),
        "partners": draw_partners(jax.random.fold_in(seeds[7], 71), 0),
    }


learn_rate = 0.3
epsilon = 1e-06

def adagrad(param, accum, grad):
    accum = accum + grad * grad
    return (param - learn_rate * grad / (jnp.sqrt(accum) + epsilon), accum)

def take_block(source, picked):
    return lax.dynamic_slice_in_dim(source, (picked * BLOCK).astype(jnp.int32), BLOCK, 0)

def put_block(source, update, picked):
    return lax.dynamic_update_slice_in_dim(source, update, (picked * BLOCK).astype(jnp.int32), 0)

def group_step(operands, sub_batch):
    users, uaccum, items, iaccum, picked, targets = operands
    user_span = USR_DEV // INNER
    first_user = sub_batch * user_span
    chosen = jax.vmap(take_block)(items, picked)
    chosen_acc = jax.vmap(take_block)(iaccum, picked)
    gathered = chosen.reshape(N_GRP * BLOCK, D)
    user_rows = users[:, first_user:first_user + user_span]
    user_acc = uaccum[:, first_user:first_user + user_span]
    scores = jnp.einsum('gud,bd->gub', user_rows, gathered, precision=lax.Precision.HIGHEST)
    softmax_rows = jax.nn.softmax(scores, axis=-1)
    onehot = (targets[:, :, None] == jnp.arange(N_GRP * BLOCK, dtype=jnp.int32)[None, None, :]).astype(jnp.float32)
    score_grad = softmax_rows - onehot
    grad_user = jnp.einsum('gub,bd->gud', score_grad, gathered, precision=lax.Precision.HIGHEST)
    grad_item = jnp.einsum('gub,gud->bd', score_grad, user_rows, precision=lax.Precision.HIGHEST).reshape(N_GRP, BLOCK, D)
    new_rows, new_acc = adagrad(user_rows, user_acc, grad_user)
    users = users.at[:, first_user:first_user + user_span].set(new_rows)
    uaccum = uaccum.at[:, first_user:first_user + user_span].set(new_acc)
    new_items, new_iacc = adagrad(chosen, chosen_acc, grad_item)
    items = jax.vmap(put_block)(items, new_items, picked)
    iaccum = jax.vmap(put_block)(iaccum, new_iacc, picked)
    return (users, uaccum, items, iaccum)

def regroup(source, per_device):
    return source.reshape(N_GRP, N_DOM, per_device, D).transpose(1, 0, 2, 3)

def restore(source):
    return source.transpose(1, 0, 2, 3).reshape(-1, D)

def reference(user_table, user_accum, item_table, item_accum, block_pick, positives, partners):
    user_span = USR_DEV // INNER
    users = regroup(user_table, USR_DEV)
    uaccum = regroup(user_accum, USR_DEV)
    items = regroup(item_table, ITEM_DEV)
    iaccum = regroup(item_accum, ITEM_DEV)
    for bucket in range(BUCKETS):
        for sub_batch in range(INNER):
            picked = block_pick[bucket, sub_batch].reshape(N_GRP, N_DOM).T
            targets = positives[bucket, sub_batch].reshape(N_GRP, N_DOM, user_span).transpose(1, 0, 2)
            users, uaccum, items, iaccum = lax.map(lambda operands: group_step(operands, sub_batch), (users, uaccum, items, iaccum, picked, targets))
        partner_row = partners[bucket].astype(jnp.int32)
        items = items[partner_row]
        iaccum = iaccum[partner_row]
    return (restore(users), restore(uaccum), restore(items), restore(iaccum))
```

```python
import functools

import jax
import jax.numpy as jnp
from jax import lax
from jax.experimental import pallas as pl
from jax.experimental.pallas import tpu as pltpu
from jax.sharding import PartitionSpec as P

BLOCK = 128
BUCKETS = 2
INNER = 2


learn_rate = 0.3
epsilon = 1e-06

HIGH = lax.Precision.HIGH
HIGHEST = lax.Precision.HIGHEST


def adagrad(param, accum, grad):
    accum = accum + grad * grad
    return (param - learn_rate * grad / (jnp.sqrt(accum) + epsilon), accum)


def each(count, body):
    lax.fori_loop(0, count, lambda n, carry: (body(n), carry)[1], 0)


def order_of(trained, wanted, keys_s, places_s, order_s):
    count = keys_s.shape[0]

    def key(b):
        found = jnp.where(trained[0] == b, 1, 0)
        found = jnp.where(trained[1] == b, 2, found)
        found = jnp.where(wanted[0] == b, 3, found)
        keys_s[b] = jnp.where(wanted[1] == b, 4, found)

    def place(b):
        own = keys_s[b] * count + b
        places_s[b] = sum(jnp.where(keys_s[o] * count + o < own, 1, 0) for o in range(count))

    def block(s):
        order_s[s] = sum(jnp.where(places_s[b] == s, b, 0) for b in range(1, count))

    each(count, key)
    each(count, place)
    if order_s is not None:
        each(count, block)


def split(value, parts):
    for part in parts:
        cut = value.astype(jnp.bfloat16)
        part[...] = cut
        value = value - cut.astype(jnp.float32)


def product(pairs, dims):
    total = None
    for a, b in pairs:
        term = lax.dot_general(a, b, (dims, ((), ())), preferred_element_type=jnp.float32)
        total = term if total is None else total + term
    return total


def train_kernel(
    first, second, early,
    picks_s, picks_v, targets_v, users_h, uacc_h, items_h, iacc_h,
    users_o, uacc_o, items_o, iacc_o,
    users, uacc, items, iacc, tags_v, tags_s, keys_s, places_s, order_s, outbox, inbox, leg_out, leg_in, last_out,
    vv, va, gg, g_in, new, done, u3, v3, score, g2,
    load_sem, store_sem, tag_sem, send_sem, recv_sem,
):
    g = lax.axis_index("grp")
    d = lax.axis_index("dom")
    final = first ^ second
    blocks = items_h.shape[0]
    span = users_h.shape[0] // INNER
    batch = 2 * BLOCK
    direct = blocks - 2
    chunk = 32

    def at_dom(mask):
        there = d
        for bit in range(8):
            if mask >> bit & 1:
                there = there + (1 - 2 * ((d // (1 << bit)) % 2)) * (1 << bit)
        return {"grp": g, "dom": there}

    across = {"grp": 1 - g, "dom": d}
    hop1, hop2 = at_dom(first), at_dom(second)
    hopf = at_dom(final) if final else None

    def load(source, target, k):
        copy = pltpu.make_async_copy(source, target, load_sem.at[k])
        copy.start()
        return copy

    loads = [
        load(items_h, items, 0),
        load(users_h.at[pl.ds(0, span)], users.at[pl.ds(0, span)], 1),
        load(iacc_h, iacc, 2),
        load(users_h.at[pl.ds(span, span)], users.at[pl.ds(span, span)], 3),
        load(uacc_h.at[pl.ds(0, span)], uacc.at[pl.ds(0, span)], 4),
        load(uacc_h.at[pl.ds(span, span)], uacc.at[pl.ds(span, span)], 5),
    ]

    def remote(source, target, k, where):
        return pltpu.make_async_remote_copy(
            source, target, send_sem.at[k], recv_sem.at[k], device_id=where, device_id_type=pl.DeviceIdType.MESH
        )

    ask = [remote(picks_v, tags_v.at[0], 0, hop1)]
    if final:
        ask += [remote(picks_v, tags_v.at[1], 1, hop2), remote(picks_v, tags_v.at[2], 2, hopf)]

    def show(k):
        return remote(vv.at[k, 0], vv.at[k, 1], 3 + k, across)

    def share(k):
        return remote(gg.at[k, 0], g_in.at[k], 7 + k, across)

    def bulk(s):
        return remote(outbox.at[s], inbox.at[s], 11 + s, hopf)

    leg_rows = remote(leg_out.at[0, 0], vv.at[2, 0], 20, hop1)
    leg_acc = remote(leg_out.at[0, 1], va.at[2], 21, hop1)
    leg_next = remote(leg_out.at[1], leg_in, 22, hop1)
    end_early = remote(last_out, inbox.at[direct], 23, hop2)
    end_late = remote(new.at[3], inbox.at[direct + 1], 24, hop2)

    barrier = pltpu.get_barrier_semaphore()
    peers = [across, hop1] + ([hop2, hopf] if final else [])
    for where in peers:
        pl.semaphore_signal(barrier, inc=1, device_id=where, device_id_type=pl.DeviceIdType.MESH)
    pl.semaphore_wait(barrier, len(peers))
    for copy in ask:
        copy.start()

    mine = [picks_s[0, k] for k in range(4)]
    again = mine[2] == mine[3]
    parts = BLOCK // chunk

    def rows_of(c):
        return pl.ds(pl.multiple_of(c * chunk, chunk), chunk)

    loads[0].wait()

    def first_rows(c):
        vv[0, 0, rows_of(c)] = items[mine[0], rows_of(c)]

    each(parts, first_rows)
    show(0).start()
    loads[2].wait()

    def first_acc(c):
        va[0, rows_of(c)] = iacc[mine[0], rows_of(c)]

    each(parts, first_acc)

    for n, tag in enumerate(ask):
        tag.wait_recv()
        pltpu.make_async_copy(tags_v.at[n], tags_s.at[n], tag_sem.at[n]).start()
    for n, tag in enumerate(ask):
        pltpu.make_async_copy(tags_v.at[n], tags_s.at[n], tag_sem.at[n]).wait()
    wanted = [tags_s[0, 0, 2], tags_s[0, 0, 3]]
    order_of(mine[:2], wanted, keys_s, places_s, order_s)
    filler = jnp.where(wanted[0] == wanted[1], order_s[blocks - 2], wanted[1])
    if final:
        order_of([tags_s[2, 0, 0], tags_s[2, 0, 1]], [tags_s[1, 0, 2], tags_s[1, 0, 3]], keys_s, places_s, None)

    def gather(pick, upto, rows_to, acc_to):
        def body(c):
            at = rows_of(c)
            rows, acc = items[pick, at], iacc[pick, at]
            for k in range(upto):
                hit = mine[k] == pick
                rows = jnp.where(hit, new[k, 0, at], rows)
                acc = jnp.where(hit, new[k, 1, at], acc)
            rows_to[at] = rows
            acc_to[at] = acc

        each(parts, body)

    def post(s, upto):
        box = outbox if final else inbox
        gather(order_s[s], upto, box.at[s, 0], box.at[s, 1])
        if final:
            bulk(s).start()

    each(early, lambda s: post(s, 0))

    row = lax.broadcasted_iota(jnp.int32, (batch, BLOCK), 0)
    nt, nn, tn = ((1,), (1,)), ((1,), (0,)), ((0,), (0,))

    def store(k, n):
        rows_u = pl.ds(pl.multiple_of((k % INNER) * span, span), span)
        source, target = ((users, users_o), (uacc, uacc_o))[n]
        return pltpu.make_async_copy(source.at[rows_u], target.at[rows_u], store_sem.at[2 * (k % INNER) + n])

    def step(k):
        base = (k % INNER) * span
        for i in range(INNER):
            @pl.when(k == i)
            def _():
                loads[1 + 2 * i].wait()

        def split_users(t):
            at = pl.ds(pl.multiple_of(t * BLOCK, BLOCK), BLOCK)
            split(users[pl.ds(pl.multiple_of(base + t * BLOCK, BLOCK), BLOCK)], [u3.at[n, at] for n in range(3)])

        each(span // BLOCK, split_users)

        def score_half(h):
            @pl.when(h == 1)
            def _():
                show(k).wait_recv()

            at = pl.ds(pl.multiple_of(h * BLOCK, BLOCK), BLOCK)
            split(vv[k, h], [v3.at[n, at] for n in range(3)])

            def tile(t):
                cols = pl.ds(pl.multiple_of(t * batch, batch), batch)
                v = [v3[n, at] for n in range(3)]
                u = [u3[n, cols] for n in range(3)]
                score[at, cols] = product(
                    [(v[2], u[0]), (v[0], u[2]), (v[1], u[1]), (v[1], u[0]), (v[0], u[1]), (v[0], u[0])], nt
                )

            each(span // batch, tile)

        each(2, score_half)

        def soften(t):
            cols = pl.ds(pl.multiple_of(t * BLOCK, BLOCK), BLOCK)
            s = score[:, cols]
            e = jnp.exp(s - jnp.max(s, 0, keepdims=True))
            target = (targets_v[k, :, cols] - g * BLOCK) & (batch - 1)
            grad = e * (1.0 / jnp.sum(e, 0, keepdims=True)) - jnp.where(row == target, 1.0, 0.0)
            split(grad, [g2.at[n, :, cols] for n in range(2)])

        each(span // BLOCK, soften)

        def item_part(h):
            at = pl.ds(pl.multiple_of((1 - h) * BLOCK, BLOCK), BLOCK)
            hi, lo = g2[0, at], g2[1, at]
            gg[k, h] = product([(lo, u3[0]), (hi, u3[1]), (hi, u3[0])], nn)

            @pl.when(h == 0)
            def _():
                share(k).start()

        each(2, item_part)
        for i in range(INNER):
            @pl.when(k == i)
            def _():
                loads[4 + i].wait()

        def user_part(t):
            cols = pl.ds(pl.multiple_of(t * BLOCK, BLOCK), BLOCK)
            at = pl.ds(pl.multiple_of(base + t * BLOCK, BLOCK), BLOCK)
            hi, lo = g2[0, :, cols], g2[1, :, cols]
            grad = product([(lo, v3[0]), (hi, v3[1]), (hi, v3[0])], tn)
            users[at], uacc[at] = adagrad(users[at], uacc[at], grad)

        each(span // BLOCK, user_part)

        @pl.when(k >= INNER)
        def _():
            store(k, 0).start()
            store(k, 1).start()

        @pl.when(k == 2)
        def _():
            leg_acc.wait_recv()

        share(k).wait_recv()

        def item_rows(c):
            at = rows_of(c)
            new[k, 0, at], new[k, 1, at] = adagrad(vv[k, 0, at], va[k, at], gg[k, 1, at] + g_in[k, at])

        each(parts, item_rows)

        @pl.when(k == 0)
        def _():
            gather(mine[1], 1, vv.at[1, 0], va.at[1])
            show(1).start()

        @pl.when(k == 1)
        def _():
            gather(wanted[0], 2, leg_out.at[0, 0], leg_out.at[0, 1])
            leg_rows.start()
            leg_acc.start()
            gather(filler, 2, leg_out.at[1, 0], leg_out.at[1, 1])
            leg_next.start()
            each(direct - early, lambda s: post(s + early, 2))
            leg_rows.wait_recv()
            show(2).start()

        @pl.when(k == 2)
        def _():
            leg_next.wait_recv()

            def next_rows(c):
                at = rows_of(c)
                vv[3, 0, at] = jnp.where(again, new[2, 0, at], leg_in[0, at])

            each(parts, next_rows)
            show(3).start()

            def next_acc(c):
                at = rows_of(c)
                va[3, at] = jnp.where(again, new[2, 1, at], leg_in[1, at])
                for n in range(2):
                    last_out[n, at] = jnp.where(again, leg_in[n, at], new[2, n, at])

            each(parts, next_acc)
            end_early.start()

        @pl.when(k == 3)
        def _():
            end_late.start()

    each(BUCKETS * INNER, step)

    if final:
        each(direct, lambda s: bulk(s).wait_recv())
    end_early.wait_recv()
    end_late.wait_recv()

    def settle(b, n):
        return pltpu.make_async_copy(
            done.at[n, b], (items_o, iacc_o)[n].at[b], store_sem.at[2 * INNER + 2 * b + n]
        )

    def unpack(b):
        source = places_s[b]

        def part(c):
            at = rows_of(c)
            for n in range(2):
                done[n, b, at] = inbox[source, n, at]

        each(parts, part)
        settle(b, 0).start()
        settle(b, 1).start()

    each(blocks, unpack)

    for copy in ask:
        copy.wait_send()
    each(BUCKETS * INNER, lambda k: (show(k).wait_send(), share(k).wait_send())[0])
    if final:
        each(direct, lambda s: bulk(s).wait_send())
    for copy in (leg_rows, leg_acc, leg_next, end_early, end_late):
        copy.wait_send()
    for n in range(2):
        each(INNER, lambda i: store(i, n).wait())
        each(blocks, lambda b: settle(b, n).wait())


def train_call(first, second, number, early, operands):
    picks, targets, user_table, user_accum, item_table, item_accum = operands
    rows, width = user_table.shape
    item_rows = item_table.shape[0]
    blocks = item_rows // BLOCK
    span = rows // INNER
    steps = BUCKETS * INNER
    f32, bf16 = jnp.float32, jnp.bfloat16
    any_space = pl.BlockSpec(memory_space=pl.ANY)
    in_vmem = pl.BlockSpec(memory_space=pltpu.VMEM)
    tile = jnp.zeros((8, 128), jnp.int32).at[0, :steps].set(picks[0])
    by_block = (blocks, BLOCK, width)
    pair = (2, BLOCK, width)
    out = pl.pallas_call(
        functools.partial(train_kernel, first, second, early),
        out_shape=(
            jax.ShapeDtypeStruct((rows, width), f32),
            jax.ShapeDtypeStruct((rows, width), f32),
            jax.ShapeDtypeStruct(by_block, f32),
            jax.ShapeDtypeStruct(by_block, f32),
        ),
        in_specs=[pl.BlockSpec(memory_space=pltpu.SMEM), in_vmem, in_vmem] + [any_space] * 4,
        out_specs=[any_space] * 4,
        scratch_shapes=[
            pltpu.VMEM((rows, width), f32),
            pltpu.VMEM((rows, width), f32),
            pltpu.VMEM(by_block, f32),
            pltpu.VMEM(by_block, f32),
            pltpu.VMEM((3, 8, 128), jnp.int32),
            pltpu.SMEM((3, 8, 128), jnp.int32),
            pltpu.SMEM((blocks,), jnp.int32),
            pltpu.SMEM((blocks,), jnp.int32),
            pltpu.SMEM((blocks,), jnp.int32),
            pltpu.VMEM((blocks - 2,) + pair, f32),
            pltpu.VMEM((blocks,) + pair, f32),
            pltpu.VMEM((2,) + pair, f32),
            pltpu.VMEM(pair, f32),
            pltpu.VMEM(pair, f32),
            pltpu.VMEM((steps,) + pair, f32),
            pltpu.VMEM((steps, BLOCK, width), f32),
            pltpu.VMEM((steps,) + pair, f32),
            pltpu.VMEM((steps, BLOCK, width), f32),
            pltpu.VMEM((steps,) + pair, f32),
            pltpu.VMEM((2,) + by_block, f32),
            pltpu.VMEM((3, span, width), bf16),
            pltpu.VMEM((3, 2 * BLOCK, width), bf16),
            pltpu.VMEM((2 * BLOCK, span), f32),
            pltpu.VMEM((2, 2 * BLOCK, span), bf16),
            pltpu.SemaphoreType.DMA((6,)),
            pltpu.SemaphoreType.DMA((2 * INNER + 2 * blocks,)),
            pltpu.SemaphoreType.DMA((3,)),
            pltpu.SemaphoreType.DMA((25,)),
            pltpu.SemaphoreType.DMA((25,)),
        ],
        compiler_params=pltpu.CompilerParams(
            collective_id=number, has_side_effects=True, vmem_limit_bytes=48 * 1024 * 1024
        ),
        name=f"train_{first}_{second}",
    )(picks, tile, targets, user_table, user_accum, item_table.reshape(by_block), item_accum.reshape(by_block))
    return out[0], out[1], out[2].reshape(item_rows, width), out[3].reshape(item_rows, width)


def kernel_body(user_table, user_accum, item_table, item_accum, block_pick, positives, partners):
    count = lax.axis_size("dom")
    levels = count.bit_length() - 1
    masks = partners[:, 0]
    level = sum((masks >> bit & 1) * bit for bit in range(levels))
    picks = block_pick.reshape(1, BUCKETS * INNER)
    targets = positives.reshape(BUCKETS * INNER, 1, -1)
    branches = []
    for first in range(levels):
        for second in range(levels):
            early = 4 if first == second else 3
            branches.append(
                lambda *operands, a=first, b=second, e=early: train_call(1 << a, 1 << b, a * levels + b, e, operands)
            )
    return lax.switch(
        level[0] * levels + level[1], branches, picks, targets, user_table, user_accum, item_table, item_accum
    )


def trade(block, mask):
    if mask == 0:
        return block
    return lax.ppermute(block, "dom", [(d, d ^ mask) for d in range(lax.axis_size("dom"))])


def train(user_rows, user_acc, chosen, chosen_acc, targets):
    gathered = lax.all_gather(chosen, "grp", axis=0, tiled=True)
    scores = jnp.einsum("ud,bd->ub", user_rows, gathered, precision=HIGHEST)
    onehot = (targets[:, None] == jnp.arange(gathered.shape[0], dtype=jnp.int32)[None, :]).astype(jnp.float32)
    score_grad = jax.nn.softmax(scores, axis=-1) - onehot
    part = jnp.einsum("ub,ud->bd", score_grad, user_rows, precision=HIGH)
    grad_item = lax.psum_scatter(part, "grp", scatter_dimension=0, tiled=True)
    grad_user = jnp.einsum("ub,bd->ud", score_grad, gathered, precision=HIGH)
    return adagrad(user_rows, user_acc, grad_user) + adagrad(chosen, chosen_acc, grad_item)


def take(table, pick):
    return lax.dynamic_slice_in_dim(table, pick * BLOCK, BLOCK, 0)


def put(table, block, pick):
    return lax.dynamic_update_slice_in_dim(table, block, pick * BLOCK, 0)


def newest(tables, updates, pick):
    found = tuple(take(table, pick) for table in tables)
    for at, blocks in updates:
        found = tuple(jnp.where(pick == at, new, old) for new, old in zip(blocks, found))
    return found


def by_level(operands, level, masks):
    branches = [lambda *arrays, mask=mask: tuple(trade(a, mask) for a in arrays) for mask in masks]
    return lax.switch(level, branches, *operands)


def plain_body(user_table, user_accum, item_table, item_accum, block_pick, positives, partners):
    position = lax.axis_index("dom")
    count = lax.axis_size("dom")
    levels = count.bit_length() - 1
    masks = jnp.bitwise_xor(partners[:, position], position)
    level = sum((masks >> bit & 1) * bit for bit in range(levels))
    singles = [1 << bit for bit in range(levels)]
    picks = block_pick[:, :, 0]
    wanted = by_level((picks,), level[0], singles)[0]
    tables = (item_table, item_accum)
    users = list(jnp.split(user_table, INNER))
    uaccs = list(jnp.split(user_accum, INNER))

    updates = []
    for i in range(INNER):
        pick = picks[0, i]
        rows, acc = newest(tables, updates, pick)
        users[i], uaccs[i], rows, acc = train(users[i], uaccs[i], rows, acc, positives[0, i])
        updates.append((pick, (rows, acc)))
    sent = []
    for i in range(INNER):
        sent += newest(tables, updates, wanted[1, i])
    came = by_level((jnp.concatenate(sent),), level[0], singles)[0]
    came = jnp.split(came, 2 * INNER)
    full = list(tables)
    for at, blocks in updates:
        full = [put(table, block, at) for table, block in zip(full, blocks)]

    updates = []
    for i in range(INNER):
        pick = picks[1, i]
        rows, acc = came[2 * i : 2 * i + 2]
        for at, blocks in updates:
            rows, acc = (jnp.where(pick == at, new, old) for new, old in zip(blocks, (rows, acc)))
        users[i], uaccs[i], rows, acc = train(users[i], uaccs[i], rows, acc, positives[1, i])
        updates.append((pick, (rows, acc)))
    late = jnp.concatenate([part for _, blocks in updates for part in blocks])

    def leave(first, second, table, accum, late, picks):
        return (
            trade(table, first ^ second),
            trade(accum, first ^ second),
            trade(late, second),
            trade(picks, second),
        )

    *bulk, late, last_picks = lax.switch(
        level[0] * levels + level[1],
        [functools.partial(leave, first, second) for first in singles for second in singles],
        *full,
        late,
        picks,
    )
    late = jnp.split(late, 2 * INNER)
    for i in range(INNER):
        bulk = [put(t, b, last_picks[1, i]) for t, b in zip(bulk, late[2 * i : 2 * i + 2])]
    return (jnp.concatenate(users, axis=0), jnp.concatenate(uaccs, axis=0), bulk[0], bulk[1])


def solution(mesh):
    rows = P(("grp", "dom"), None)
    columns = P(None, None, ("grp", "dom"))
    return jax.shard_map(
        kernel_body if mesh.shape["grp"] == 2 else plain_body,
        mesh=mesh,
        in_specs=(rows, rows, rows, rows, columns, columns, P()),
        out_specs=(rows, rows, rows, rows),
        check_vma=False,
    )
```

```python
import functools

import jax
import jax.numpy as jnp
from jax import lax
from jax.experimental import pallas as pl
from jax.experimental.pallas import tpu as pltpu
from jax.sharding import PartitionSpec as P

BLOCK = 128
BUCKETS = 2
INNER = 2


learn_rate = 0.3
epsilon = 1e-06

HIGH = lax.Precision.HIGH
HIGHEST = lax.Precision.HIGHEST


def adagrad(param, accum, grad):
    accum = accum + grad * grad
    return (param - learn_rate * grad / (jnp.sqrt(accum) + epsilon), accum)


def each(count, body):
    lax.fori_loop(0, count, lambda n, carry: (body(n), carry)[1], 0)


def order_of(trained, wanted, keys_s, places_s, order_s):
    count = keys_s.shape[0]

    def key(b):
        found = jnp.where(trained[0] == b, 1, 0)
        found = jnp.where(trained[1] == b, 2, found)
        found = jnp.where(wanted[0] == b, 3, found)
        keys_s[b] = jnp.where(wanted[1] == b, 4, found)

    def place(b):
        own = keys_s[b] * count + b
        places_s[b] = sum(jnp.where(keys_s[o] * count + o < own, 1, 0) for o in range(count))

    def block(s):
        order_s[s] = sum(jnp.where(places_s[b] == s, b, 0) for b in range(1, count))

    each(count, key)
    each(count, place)
    if order_s is not None:
        each(count, block)


def split(value, parts):
    for part in parts:
        cut = value.astype(jnp.bfloat16)
        part[...] = cut
        value = value - cut.astype(jnp.float32)


def product(pairs, dims):
    total = None
    for a, b in pairs:
        term = lax.dot_general(a, b, (dims, ((), ())), preferred_element_type=jnp.float32)
        total = term if total is None else total + term
    return total


def train_kernel(
    first, second, early,
    picks_s, targets_h, users_h, uacc_h, items_h, iacc_h,
    items_o, iacc_o, users, uacc_o,
    uacc, table, targets, tag, tags_v, tags_s, keys_s, places_s, order_s, outbox, inbox, leg_out, leg_in, last_out,
    vv, va, gg, g_in, new, u3, v3, score, g2,
    load_sem, store_sem, tag_sem, send_sem, recv_sem,
):
    g = lax.axis_index("grp")
    d = lax.axis_index("dom")
    final = first ^ second
    blocks = items_h.shape[0]
    span = users_h.shape[0] // INNER
    batch = 2 * BLOCK
    halves = 2 * (blocks - 2)
    chunk = 32
    parts = BLOCK // chunk

    def at_dom(mask):
        there = d
        for bit in range(8):
            if mask >> bit & 1:
                there = there + (1 - 2 * ((d // (1 << bit)) % 2)) * (1 << bit)
        return {"grp": g, "dom": there}

    across = {"grp": 1 - g, "dom": d}
    hop1, hop2 = at_dom(first), at_dom(second)
    hopf = at_dom(final) if final else None

    def load(source, target, k):
        copy = pltpu.make_async_copy(source, target, load_sem.at[k])
        copy.start()
        return copy

    loads = [
        load(items_h, table.at[0], 0),
        load(iacc_h, table.at[1], 2),
        load(users_h.at[pl.ds(0, span)], users.at[pl.ds(0, span)], 1),
        load(users_h.at[pl.ds(span, span)], users.at[pl.ds(span, span)], 3),
        load(uacc_h.at[pl.ds(0, span)], uacc.at[pl.ds(0, span)], 4),
        load(uacc_h.at[pl.ds(span, span)], uacc.at[pl.ds(span, span)], 5),
    ]

    def remote(source, target, k, where):
        return pltpu.make_async_remote_copy(
            source, target, send_sem.at[k], recv_sem.at[k], device_id=where, device_id_type=pl.DeviceIdType.MESH
        )

    def rows_of(c):
        return pl.ds(pl.multiple_of(c * chunk, chunk), chunk)

    ask = [remote(tag, tags_v.at[0], 0, hop1)]
    if final:
        ask += [remote(tag, tags_v.at[1], 1, hop2), remote(tag, tags_v.at[2], 2, hopf)]

    def show(k, c):
        return remote(vv.at[k, 0, rows_of(c)], vv.at[k, 1, rows_of(c)], 3 + k * parts + c, across)

    def share(k, c):
        return remote(gg.at[k, 0, rows_of(c)], g_in.at[k, rows_of(c)], 3 + (4 + k) * parts + c, across)

    sem = 3 + 8 * parts

    def leg_rows(c):
        return remote(leg_out.at[0, 0, rows_of(c)], vv.at[2, 0, rows_of(c)], sem + c, hop1)

    def end_late(n, c):
        return remote(
            new.at[3, n, rows_of(c)], inbox.at[blocks - 1, n, rows_of(c)], sem + (1 + n) * parts + c, hop2
        )

    sem_bulk = sem + 3 * parts

    def bulk(h):
        return remote(outbox.at[h // 2, h % 2], inbox.at[h // 2, h % 2], sem_bulk + h, hopf)

    sem_leg = sem_bulk + halves
    leg_acc = remote(leg_out.at[0, 1], va.at[2], sem_leg, hop1)
    next_rows = remote(leg_out.at[1, 0], leg_in.at[0], sem_leg + 1, hop1)
    next_acc = remote(leg_out.at[1, 1], leg_in.at[1], sem_leg + 2, hop1)
    end_early = remote(last_out, inbox.at[blocks - 2], sem_leg + 3, hop2)

    mine = [picks_s[k // INNER, k % INNER, 0] for k in range(BUCKETS * INNER)]
    lane = lax.broadcasted_iota(jnp.int32, tag.shape, 1)
    told = jnp.zeros(tag.shape, jnp.int32)
    for k in range(BUCKETS * INNER):
        told = jnp.where(lane == k, mine[k], told)
        targets[k] = targets_h[k // INNER, pl.ds(k % INNER, 1)]
    tag[...] = told

    barrier = pltpu.get_barrier_semaphore()
    peers = [across, hop1] + ([hop2, hopf] if final else [])
    for where in peers:
        pl.semaphore_signal(barrier, inc=1, device_id=where, device_id_type=pl.DeviceIdType.MESH)
    loads[0].wait()
    loads[1].wait()
    each(parts, lambda c: put_rows(vv.at[0, 0, rows_of(c)], table[0, mine[0], rows_of(c)]))
    pl.semaphore_wait(barrier, len(peers))
    for copy in ask:
        copy.start()
    each(parts, lambda c: show(0, c).start())
    again = mine[2] == mine[3]

    each(parts, lambda c: put_rows(va.at[0, rows_of(c)], table[1, mine[0], rows_of(c)]))

    for n, copy in enumerate(ask):
        copy.wait_recv()
        pltpu.make_async_copy(tags_v.at[n], tags_s.at[n], tag_sem.at[n]).start()
    for n, copy in enumerate(ask):
        pltpu.make_async_copy(tags_v.at[n], tags_s.at[n], tag_sem.at[n]).wait()
    wanted = [tags_s[0, 0, 2], tags_s[0, 0, 3]]
    order_of(mine[:2], wanted, keys_s, places_s, order_s)
    filler = jnp.where(wanted[0] == wanted[1], order_s[blocks - 2], wanted[1])
    def newest(pick, n, at, upto):
        value = table[n, pick, at]
        for k in range(upto):
            value = jnp.where(mine[k] == pick, new[k, n, at], value)
        return value

    def gather(pick, n, upto, target):
        each(parts, lambda c: put_rows(target.at[rows_of(c)], newest(pick, n, rows_of(c), upto)))

    def post(h, upto):
        box = outbox if final else inbox
        gather(order_s[h // 2], h % 2, upto, box.at[h // 2, h % 2])
        if final:
            bulk(h).start()

    each(early, lambda h: post(h, 0))
    if final:
        order_of([tags_s[2, 0, 0], tags_s[2, 0, 1]], [tags_s[1, 0, 2], tags_s[1, 0, 3]], keys_s, places_s, None)

    row = lax.broadcasted_iota(jnp.int32, (batch, BLOCK), 0)
    nt, nn, tn = ((1,), (1,)), ((1,), (0,)), ((0,), (0,))

    def store(i):
        rows_u = pl.ds(pl.multiple_of(i * span, span), span)
        return pltpu.make_async_copy(uacc.at[rows_u], uacc_o.at[rows_u], store_sem.at[i])

    def step(k):
        base = (k % INNER) * span
        for i in range(INNER):
            @pl.when(k == i)
            def _():
                loads[2 + i].wait()

        def split_users(t):
            at = pl.ds(pl.multiple_of(t * BLOCK, BLOCK), BLOCK)
            split(users[pl.ds(pl.multiple_of(base + t * BLOCK, BLOCK), BLOCK)], [u3.at[n, at] for n in range(3)])

        each(span // BLOCK, split_users)

        def score_half(h):
            def split_items(c):
                @pl.when(h == 1)
                def _():
                    show(k, c).wait_recv()

                at = pl.ds(pl.multiple_of(h * BLOCK + c * chunk, chunk), chunk)
                split(vv[k, h, rows_of(c)], [v3.at[n, at] for n in range(3)])

            each(parts, split_items)
            at = pl.ds(pl.multiple_of(h * BLOCK, BLOCK), BLOCK)

            def tile(t):
                cols = pl.ds(pl.multiple_of(t * batch, batch), batch)
                v = [v3[n, at] for n in range(3)]
                u = [u3[n, cols] for n in range(3)]
                score[at, cols] = product(
                    [(v[2], u[0]), (v[0], u[2]), (v[1], u[1]), (v[1], u[0]), (v[0], u[1]), (v[0], u[0])], nt
                )

            each(span // batch, tile)

        each(2, score_half)

        def soften(t):
            cols = pl.ds(pl.multiple_of(t * BLOCK, BLOCK), BLOCK)
            s = score[:, cols]
            e = jnp.exp(s - jnp.max(s, 0, keepdims=True))
            target = (targets[k, :, cols] - g * BLOCK) & (batch - 1)
            grad = e * (1.0 / jnp.sum(e, 0, keepdims=True)) - jnp.where(row == target, 1.0, 0.0)
            split(grad, [g2.at[n, :, cols] for n in range(2)])

        each(span // BLOCK, soften)

        def item_part(h):
            at = pl.ds(pl.multiple_of((1 - h) * BLOCK, BLOCK), BLOCK)
            hi, lo = g2[0, at], g2[1, at]
            gg[k, h] = product([(lo, u3[0]), (hi, u3[1]), (hi, u3[0])], nn)

            @pl.when(h == 0)
            def _():
                each(parts, lambda c: share(k, c).start())

        each(2, item_part)
        for i in range(INNER):
            @pl.when(k == i)
            def _():
                loads[4 + i].wait()

        def user_part(t):
            cols = pl.ds(pl.multiple_of(t * BLOCK, BLOCK), BLOCK)
            at = pl.ds(pl.multiple_of(base + t * BLOCK, BLOCK), BLOCK)
            hi, lo = g2[0, :, cols], g2[1, :, cols]
            grad = product([(lo, v3[0]), (hi, v3[1]), (hi, v3[0])], tn)
            users[at], uacc[at] = adagrad(users[at], uacc[at], grad)

        each(span // BLOCK, user_part)

        @pl.when(k >= INNER)
        def _():
            store(k % INNER).start()

        @pl.when(k == 2)
        def _():
            next_rows.wait_recv()
            leg_acc.wait_recv()

        def item_rows(c):
            at = rows_of(c)
            share(k, c).wait_recv()
            new[k, 0, at], new[k, 1, at] = adagrad(vv[k, 0, at], va[k, at], gg[k, 1, at] + g_in[k, at])

            @pl.when(k == 0)
            def _():
                vv[1, 0, at] = newest(mine[1], 0, at, 1)
                show(1, c).start()

            @pl.when(k == 1)
            def _():
                leg_out[0, 0, at] = newest(wanted[0], 0, at, 2)
                leg_rows(c).start()

            @pl.when(k == 2)
            def _():
                vv[3, 0, at] = jnp.where(again, new[2, 0, at], leg_in[0, at])
                show(3, c).start()

            @pl.when(k == 3)
            def _():
                end_late(0, c).start()
                end_late(1, c).start()

        each(parts, item_rows)

        @pl.when(k == 0)
        def _():
            gather(mine[1], 1, 1, va.at[1])

        @pl.when(k == 1)
        def _():
            gather(filler, 0, 2, leg_out.at[1, 0])
            next_rows.start()

            def relay(c):
                leg_rows(c).wait_recv()
                show(2, c).start()

            each(parts, relay)
            gather(wanted[0], 1, 2, leg_out.at[0, 1])
            leg_acc.start()
            gather(filler, 1, 2, leg_out.at[1, 1])
            next_acc.start()
            each(halves - early, lambda h: post(h + early, 2))

        @pl.when(k == 2)
        def _():
            next_acc.wait_recv()

            def keep(c):
                at = rows_of(c)
                va[3, at] = jnp.where(again, new[2, 1, at], leg_in[1, at])
                for n in range(2):
                    last_out[n, at] = jnp.where(again, leg_in[n, at], new[2, n, at])

            each(parts, keep)
            end_early.start()

    each(BUCKETS * INNER, step)

    for copy in ask + [leg_acc, next_rows, next_acc]:
        copy.wait_send()
    each(4 * parts, lambda q: (show(q // parts, q % parts).wait_send(), share(q // parts, q % parts).wait_send())[0])
    each(parts, lambda c: leg_rows(c).wait_send())
    if final:
        each(halves, lambda h: (bulk(h).wait_send(), bulk(h).wait_recv())[0])
    end_early.wait()
    each(parts, lambda c: (end_late(0, c).wait(), end_late(1, c).wait())[0])

    def unpack(b):
        source = places_s[b]

        def part(c):
            at = rows_of(c)
            items_o[b, at] = inbox[source, 0, at]
            iacc_o[b, at] = inbox[source, 1, at]

        each(parts, part)

    each(blocks, unpack)
    each(INNER, lambda i: store(i).wait())


def put_rows(target, value):
    target[...] = value


def flush_kernel(items, iacc, users, uacc, items_o, iacc_o, users_o, uacc_o, held, sems):
    fetch = pltpu.make_async_copy(uacc, held, sems.at[0])
    fetch.start()
    copies = [
        pltpu.make_async_copy(source, target, sems.at[1 + n])
        for n, (source, target) in enumerate(((users, users_o), (items, items_o), (iacc, iacc_o), (held, uacc_o)))
    ]
    for copy in copies[:3]:
        copy.start()
    fetch.wait()
    copies[3].start()
    for copy in copies:
        copy.wait()


def train_call(first, second, number, early, operands):
    picks, targets, user_table, user_accum, item_table, item_accum = operands
    rows, width = user_table.shape
    item_rows = item_table.shape[0]
    blocks = item_rows // BLOCK
    span = rows // INNER
    steps = BUCKETS * INNER
    sems = 3 + 11 * 4 + 2 * (blocks - 2) + 4
    f32, bf16 = jnp.float32, jnp.bfloat16
    hbm = pl.BlockSpec(memory_space=pltpu.HBM)
    in_vmem = pl.BlockSpec(memory_space=pltpu.VMEM)
    by_block = (blocks, BLOCK, width)
    pair = (2, BLOCK, width)
    return pl.pallas_call(
        functools.partial(train_kernel, first, second, early),
        out_shape=(
            jax.ShapeDtypeStruct(by_block, f32),
            jax.ShapeDtypeStruct(by_block, f32),
            jax.ShapeDtypeStruct((rows, width), f32),
            jax.ShapeDtypeStruct((rows, width), f32),
        ),
        in_specs=[pl.BlockSpec(memory_space=pltpu.SMEM), in_vmem] + [hbm] * 4,
        out_specs=[in_vmem, in_vmem, in_vmem, hbm],
        scratch_shapes=[
            pltpu.VMEM((rows, width), f32),
            pltpu.VMEM((2,) + by_block, f32),
            pltpu.VMEM((steps, 1, span), jnp.int32),
            pltpu.VMEM((8, 128), jnp.int32),
            pltpu.VMEM((3, 8, 128), jnp.int32),
            pltpu.SMEM((3, 8, 128), jnp.int32),
            pltpu.SMEM((blocks,), jnp.int32),
            pltpu.SMEM((blocks,), jnp.int32),
            pltpu.SMEM((blocks,), jnp.int32),
            pltpu.VMEM((blocks - 2,) + pair, f32),
            pltpu.VMEM((blocks,) + pair, f32),
            pltpu.VMEM((2,) + pair, f32),
            pltpu.VMEM(pair, f32),
            pltpu.VMEM(pair, f32),
            pltpu.VMEM((steps,) + pair, f32),
            pltpu.VMEM((steps, BLOCK, width), f32),
            pltpu.VMEM((steps,) + pair, f32),
            pltpu.VMEM((steps, BLOCK, width), f32),
            pltpu.VMEM((steps,) + pair, f32),
            pltpu.VMEM((3, span, width), bf16),
            pltpu.VMEM((3, 2 * BLOCK, width), bf16),
            pltpu.VMEM((2 * BLOCK, span), f32),
            pltpu.VMEM((2, 2 * BLOCK, span), bf16),
            pltpu.SemaphoreType.DMA((6,)),
            pltpu.SemaphoreType.DMA((INNER,)),
            pltpu.SemaphoreType.DMA((3,)),
            pltpu.SemaphoreType.DMA((sems,)),
            pltpu.SemaphoreType.DMA((sems,)),
        ],
        compiler_params=pltpu.CompilerParams(
            collective_id=number, has_side_effects=True, vmem_limit_bytes=20 * 1024 * 1024
        ),
        name=f"train_{first}_{second}",
    )(picks, targets, user_table, user_accum, item_table.reshape(by_block), item_accum.reshape(by_block))


def early_halves(first, second, count):
    if first == second or first == 1:
        return 8
    if count // 2 in (first, second):
        return 4
    return 5


def kernel_body(user_table, user_accum, item_table, item_accum, block_pick, positives, partners):
    count = lax.axis_size("dom")
    levels = count.bit_length() - 1
    branches = []
    for a in range(levels):
        for b in range(levels):
            early = early_halves(1 << a, 1 << b, count)
            branches.append(functools.partial(train_branch, 1 << a, 1 << b, a * levels + b, early))
    masks = partners[:, :1]
    level = sum((masks >> bit & 1) * bit for bit in range(1, levels))
    leading = lax.broadcasted_iota(jnp.int32, level.shape, 0) == 0
    trained = lax.switch(
        jnp.sum(jnp.where(leading, level * levels, level)),
        branches, block_pick, positives, user_table, user_accum, item_table, item_accum,
    )
    hbm, any_space = pl.BlockSpec(memory_space=pltpu.HBM), pl.BlockSpec(memory_space=pl.ANY)
    items, iacc, users, uacc = pl.pallas_call(
        flush_kernel,
        out_shape=tuple(jax.ShapeDtypeStruct(t.shape, t.dtype) for t in trained),
        in_specs=[any_space] * 3 + [hbm],
        out_specs=[hbm] * 4,
        scratch_shapes=[pltpu.VMEM(user_accum.shape, jnp.float32), pltpu.SemaphoreType.DMA((5,))],
        compiler_params=pltpu.CompilerParams(vmem_limit_bytes=2 * 1024 * 1024),
        name="flush",
    )(*trained)
    return users, uacc, items.reshape(item_table.shape), iacc.reshape(item_table.shape)


def train_branch(first, second, number, early, *operands):
    return train_call(first, second, number, early, operands)


def trade(block, mask):
    if mask == 0:
        return block
    return lax.ppermute(block, "dom", [(d, d ^ mask) for d in range(lax.axis_size("dom"))])


def train(user_rows, user_acc, chosen, chosen_acc, targets):
    gathered = lax.all_gather(chosen, "grp", axis=0, tiled=True)
    scores = jnp.einsum("ud,bd->ub", user_rows, gathered, precision=HIGHEST)
    onehot = (targets[:, None] == jnp.arange(gathered.shape[0], dtype=jnp.int32)[None, :]).astype(jnp.float32)
    score_grad = jax.nn.softmax(scores, axis=-1) - onehot
    part = jnp.einsum("ub,ud->bd", score_grad, user_rows, precision=HIGH)
    grad_item = lax.psum_scatter(part, "grp", scatter_dimension=0, tiled=True)
    grad_user = jnp.einsum("ub,bd->ud", score_grad, gathered, precision=HIGH)
    return adagrad(user_rows, user_acc, grad_user) + adagrad(chosen, chosen_acc, grad_item)


def take(table, pick):
    return lax.dynamic_slice_in_dim(table, pick * BLOCK, BLOCK, 0)


def put(table, block, pick):
    return lax.dynamic_update_slice_in_dim(table, block, pick * BLOCK, 0)


def newest(tables, updates, pick):
    found = tuple(take(table, pick) for table in tables)
    for at, blocks in updates:
        found = tuple(jnp.where(pick == at, new, old) for new, old in zip(blocks, found))
    return found


def by_level(operands, level, masks):
    branches = [lambda *arrays, mask=mask: tuple(trade(a, mask) for a in arrays) for mask in masks]
    return lax.switch(level, branches, *operands)


def plain_body(user_table, user_accum, item_table, item_accum, block_pick, positives, partners):
    position = lax.axis_index("dom")
    count = lax.axis_size("dom")
    levels = count.bit_length() - 1
    masks = jnp.bitwise_xor(partners[:, position], position)
    level = sum((masks >> bit & 1) * bit for bit in range(levels))
    singles = [1 << bit for bit in range(levels)]
    picks = block_pick[:, :, 0]
    wanted = by_level((picks,), level[0], singles)[0]
    tables = (item_table, item_accum)
    users = list(jnp.split(user_table, INNER))
    uaccs = list(jnp.split(user_accum, INNER))

    updates = []
    for i in range(INNER):
        pick = picks[0, i]
        rows, acc = newest(tables, updates, pick)
        users[i], uaccs[i], rows, acc = train(users[i], uaccs[i], rows, acc, positives[0, i])
        updates.append((pick, (rows, acc)))
    sent = []
    for i in range(INNER):
        sent += newest(tables, updates, wanted[1, i])
    came = by_level((jnp.concatenate(sent),), level[0], singles)[0]
    came = jnp.split(came, 2 * INNER)
    full = list(tables)
    for at, blocks in updates:
        full = [put(table, block, at) for table, block in zip(full, blocks)]

    updates = []
    for i in range(INNER):
        pick = picks[1, i]
        rows, acc = came[2 * i : 2 * i + 2]
        for at, blocks in updates:
            rows, acc = (jnp.where(pick == at, new, old) for new, old in zip(blocks, (rows, acc)))
        users[i], uaccs[i], rows, acc = train(users[i], uaccs[i], rows, acc, positives[1, i])
        updates.append((pick, (rows, acc)))
    late = jnp.concatenate([part for _, blocks in updates for part in blocks])

    def leave(first, second, table, accum, late, picks):
        return (
            trade(table, first ^ second),
            trade(accum, first ^ second),
            trade(late, second),
            trade(picks, second),
        )

    *bulk, late, last_picks = lax.switch(
        level[0] * levels + level[1],
        [functools.partial(leave, first, second) for first in singles for second in singles],
        *full,
        late,
        picks,
    )
    late = jnp.split(late, 2 * INNER)
    for i in range(INNER):
        bulk = [put(t, b, last_picks[1, i]) for t, b in zip(bulk, late[2 * i : 2 * i + 2])]
    return (jnp.concatenate(users, axis=0), jnp.concatenate(uaccs, axis=0), bulk[0], bulk[1])


def solution(mesh):
    rows = P(("grp", "dom"), None)
    columns = P(None, None, ("grp", "dom"))
    return jax.shard_map(
        kernel_body if mesh.shape["grp"] == 2 else plain_body,
        mesh=mesh,
        in_specs=(rows, rows, rows, rows, columns, columns, P()),
        out_specs=(rows, rows, rows, rows),
        check_vma=False,
    )
```

```python
import functools

import jax
import jax.numpy as jnp
from jax import lax
from jax.experimental import pallas as pl
from jax.experimental.pallas import tpu as pltpu
from jax.sharding import PartitionSpec as P

BLOCK = 128
BUCKETS = 2
INNER = 2


learn_rate = 0.3
epsilon = 1e-06

HIGH = lax.Precision.HIGH
HIGHEST = lax.Precision.HIGHEST


def adagrad(param, accum, grad):
    accum = accum + grad * grad
    return (param - learn_rate * grad / (jnp.sqrt(accum) + epsilon), accum)


def each(count, body):
    lax.fori_loop(0, count, lambda n, carry: (body(n), carry)[1], 0)


def order_of(trained, wanted, keys_s, places_s, order_s):
    count = keys_s.shape[0]

    def key(b):
        found = jnp.where(trained[0] == b, 1, 0)
        found = jnp.where(trained[1] == b, 2, found)
        found = jnp.where(wanted[0] == b, 3, found)
        keys_s[b] = jnp.where(wanted[1] == b, 4, found)

    def place(b):
        own = keys_s[b] * count + b
        places_s[b] = sum(jnp.where(keys_s[o] * count + o < own, 1, 0) for o in range(count))

    def block(s):
        order_s[s] = sum(jnp.where(places_s[b] == s, b, 0) for b in range(1, count))

    each(count, key)
    each(count, place)
    if order_s is not None:
        each(count, block)


def split(value, parts):
    for part in parts:
        cut = value.astype(jnp.bfloat16)
        part[...] = cut
        value = value - cut.astype(jnp.float32)


def product(pairs, dims):
    total = None
    for a, b in pairs:
        term = lax.dot_general(a, b, (dims, ((), ())), preferred_element_type=jnp.float32)
        total = term if total is None else total + term
    return total


def train_kernel(
    first, second, plan,
    picks_s, targets_h, users_h, uacc_h, items_h, iacc_h,
    items_o, iacc_o, users, uacc_o,
    uacc, table, raw, targets, tag, tags_v, tags_s, keys_s, places_s, order_s, outbox, inbox, leg_out, leg_in, last_out,
    vv, va, gg, g_in, new, u3, v3, score, g2,
    load_sem, store_sem, tag_sem, send_sem, recv_sem,
):
    g = lax.axis_index("grp")
    d = lax.axis_index("dom")
    final = first ^ second
    blocks = items_h.shape[0]
    span = users_h.shape[0] // INNER
    batch = 2 * BLOCK
    halves = 2 * (blocks - 2)
    chunk = 32
    parts = BLOCK // chunk

    def at_dom(mask):
        there = d
        for bit in range(8):
            if mask >> bit & 1:
                there = there + (1 - 2 * ((d // (1 << bit)) % 2)) * (1 << bit)
        return {"grp": g, "dom": there}

    across = {"grp": 1 - g, "dom": d}
    hop1, hop2 = at_dom(first), at_dom(second)
    hopf = at_dom(final) if final else None

    def load(source, target, k):
        copy = pltpu.make_async_copy(source, target, load_sem.at[k])
        copy.start()
        return copy

    loads = [
        load(items_h, table.at[0], 0),
        load(iacc_h, table.at[1], 2),
        load(users_h.at[pl.ds(0, span)], users.at[pl.ds(0, span)], 1),
        load(users_h.at[pl.ds(span, span)], users.at[pl.ds(span, span)], 3),
        load(uacc_h.at[pl.ds(0, span)], uacc.at[pl.ds(0, span)], 4),
        load(uacc_h.at[pl.ds(span, span)], uacc.at[pl.ds(span, span)], 5),
        load(targets_h, raw, 6),
    ]

    def remote(source, target, k, where):
        return pltpu.make_async_remote_copy(
            source, target, send_sem.at[k], recv_sem.at[k], device_id=where, device_id_type=pl.DeviceIdType.MESH
        )

    def rows_of(c):
        return pl.ds(pl.multiple_of(c * chunk, chunk), chunk)

    ask = [remote(tag, tags_v.at[0], 0, hop1)]
    if final:
        ask += [remote(tag, tags_v.at[1], 1, hop2), remote(tag, tags_v.at[2], 2, hopf)]

    def show(k, c):
        return remote(vv.at[k, 0, rows_of(c)], vv.at[k, 1, rows_of(c)], 3 + k * parts + c, across)

    def share(k, c):
        return remote(gg.at[k, 0, rows_of(c)], g_in.at[k, rows_of(c)], 3 + (4 + k) * parts + c, across)

    sem = 3 + 8 * parts

    def leg_rows(c):
        return remote(leg_out.at[0, 0, rows_of(c)], vv.at[2, 0, rows_of(c)], sem + c, hop1)

    def end_late(n, c):
        return remote(
            new.at[3, n, rows_of(c)], inbox.at[blocks - 1, n, rows_of(c)], sem + (1 + n) * parts + c, hop2
        )

    sem_bulk = sem + 3 * parts

    def bulk(h):
        return remote(outbox.at[h // 2, h % 2], inbox.at[h // 2, h % 2], sem_bulk + h, hopf)

    sem_leg = sem_bulk + halves
    leg_acc = remote(leg_out.at[0, 1], va.at[2], sem_leg, hop1)
    next_rows = remote(leg_out.at[1, 0], leg_in.at[0], sem_leg + 1, hop1)
    next_acc = remote(leg_out.at[1, 1], leg_in.at[1], sem_leg + 2, hop1)
    end_early = remote(last_out, inbox.at[blocks - 2], sem_leg + 3, hop2)

    mine = [picks_s[k // INNER, k % INNER, 0] for k in range(BUCKETS * INNER)]
    lane = lax.broadcasted_iota(jnp.int32, tag.shape, 1)
    told = jnp.zeros(tag.shape, jnp.int32)
    for k in range(BUCKETS * INNER):
        told = jnp.where(lane == k, mine[k], told)
    tag[...] = told

    barrier = pltpu.get_barrier_semaphore()
    peers = [across, hop1] + ([hop2, hopf] if final else [])
    for where in peers:
        pl.semaphore_signal(barrier, inc=1, device_id=where, device_id_type=pl.DeviceIdType.MESH)
    loads[0].wait()
    loads[1].wait()
    each(parts, lambda c: put_rows(vv.at[0, 0, rows_of(c)], table[0, mine[0], rows_of(c)]))
    pl.semaphore_wait(barrier, len(peers))
    for copy in ask:
        copy.start()
    each(parts, lambda c: show(0, c).start())
    again = mine[2] == mine[3]

    each(parts, lambda c: put_rows(va.at[0, rows_of(c)], table[1, mine[0], rows_of(c)]))

    for n, copy in enumerate(ask):
        copy.wait_recv()
        pltpu.make_async_copy(tags_v.at[n], tags_s.at[n], tag_sem.at[n]).start()
    for n, copy in enumerate(ask):
        pltpu.make_async_copy(tags_v.at[n], tags_s.at[n], tag_sem.at[n]).wait()
    wanted = [tags_s[0, 0, 2], tags_s[0, 0, 3]]
    order_of(mine[:2], wanted, keys_s, places_s, order_s)
    filler = jnp.where(wanted[0] == wanted[1], order_s[blocks - 2], wanted[1])
    def newest(pick, n, at, upto):
        value = table[n, pick, at]
        for k in range(upto):
            value = jnp.where(mine[k] == pick, new[k, n, at], value)
        return value

    def gather(pick, n, upto, target):
        each(parts, lambda c: put_rows(target.at[rows_of(c)], newest(pick, n, rows_of(c), upto)))

    def post(h, upto):
        box = outbox if final else inbox
        gather(order_s[h // 2], h % 2, upto, box.at[h // 2, h % 2])
        if final:
            bulk(h).start()

    each(plan[0], lambda h: post(h, 0))
    if final:
        order_of([tags_s[2, 0, 0], tags_s[2, 0, 1]], [tags_s[1, 0, 2], tags_s[1, 0, 3]], keys_s, places_s, None)

    def late_posts(group):
        if plan[group]:
            each(plan[group], lambda h: post(h + sum(plan[:group]), 2))

    loads[6].wait()
    for k in range(BUCKETS * INNER):
        targets[k] = raw[k // INNER, pl.ds(k % INNER, 1)]
    row = lax.broadcasted_iota(jnp.int32, (batch, BLOCK), 0)
    nt, nn, tn = ((1,), (1,)), ((1,), (0,)), ((0,), (0,))

    def store(i):
        rows_u = pl.ds(pl.multiple_of(i * span, span), span)
        return pltpu.make_async_copy(uacc.at[rows_u], uacc_o.at[rows_u], store_sem.at[i])

    def step(k):
        base = (k % INNER) * span
        for i in range(INNER):
            @pl.when(k == i)
            def _():
                loads[2 + i].wait()

        def split_users(t):
            at = pl.ds(pl.multiple_of(t * BLOCK, BLOCK), BLOCK)
            split(users[pl.ds(pl.multiple_of(base + t * BLOCK, BLOCK), BLOCK)], [u3.at[n, at] for n in range(3)])

        each(span // BLOCK, split_users)

        def score_half(h):
            def split_items(c):
                @pl.when(h == 1)
                def _():
                    show(k, c).wait_recv()

                at = pl.ds(pl.multiple_of(h * BLOCK + c * chunk, chunk), chunk)
                split(vv[k, h, rows_of(c)], [v3.at[n, at] for n in range(3)])

            each(parts, split_items)
            at = pl.ds(pl.multiple_of(h * BLOCK, BLOCK), BLOCK)

            def tile(t):
                cols = pl.ds(pl.multiple_of(t * batch, batch), batch)
                v = [v3[n, at] for n in range(3)]
                u = [u3[n, cols] for n in range(3)]
                score[at, cols] = product(
                    [(v[2], u[0]), (v[0], u[2]), (v[1], u[1]), (v[1], u[0]), (v[0], u[1]), (v[0], u[0])], nt
                )

            each(span // batch, tile)

        each(2, score_half)

        def soften(t):
            cols = pl.ds(pl.multiple_of(t * BLOCK, BLOCK), BLOCK)
            s = score[:, cols]
            e = jnp.exp(s - jnp.max(s, 0, keepdims=True))
            target = (targets[k, :, cols] - g * BLOCK) & (batch - 1)
            grad = e * (1.0 / jnp.sum(e, 0, keepdims=True)) - jnp.where(row == target, 1.0, 0.0)
            split(grad, [g2.at[n, :, cols] for n in range(2)])

        each(span // BLOCK, soften)

        def item_part(h):
            at = pl.ds(pl.multiple_of((1 - h) * BLOCK, BLOCK), BLOCK)
            hi, lo = g2[0, at], g2[1, at]
            gg[k, h] = product([(lo, u3[0]), (hi, u3[1]), (hi, u3[0])], nn)

            @pl.when(h == 0)
            def _():
                each(parts, lambda c: share(k, c).start())

        each(2, item_part)
        for i in range(INNER):
            @pl.when(k == i)
            def _():
                loads[4 + i].wait()

        def user_part(t):
            cols = pl.ds(pl.multiple_of(t * BLOCK, BLOCK), BLOCK)
            at = pl.ds(pl.multiple_of(base + t * BLOCK, BLOCK), BLOCK)
            hi, lo = g2[0, :, cols], g2[1, :, cols]
            grad = product([(lo, v3[0]), (hi, v3[1]), (hi, v3[0])], tn)
            users[at], uacc[at] = adagrad(users[at], uacc[at], grad)

        each(span // BLOCK, user_part)

        @pl.when(k >= INNER)
        def _():
            store(k % INNER).start()

        @pl.when(k == 2)
        def _():
            next_rows.wait_recv()
            leg_acc.wait_recv()

        def item_rows(c):
            at = rows_of(c)
            share(k, c).wait_recv()
            new[k, 0, at], new[k, 1, at] = adagrad(vv[k, 0, at], va[k, at], gg[k, 1, at] + g_in[k, at])

            @pl.when(k == 0)
            def _():
                vv[1, 0, at] = newest(mine[1], 0, at, 1)
                show(1, c).start()

            @pl.when(k == 1)
            def _():
                leg_out[0, 0, at] = newest(wanted[0], 0, at, 2)
                leg_rows(c).start()

            @pl.when(k == 2)
            def _():
                vv[3, 0, at] = jnp.where(again, new[2, 0, at], leg_in[0, at])
                show(3, c).start()

            @pl.when(k == 3)
            def _():
                end_late(0, c).start()
                end_late(1, c).start()

        each(parts, item_rows)

        @pl.when(k == 0)
        def _():
            gather(mine[1], 1, 1, va.at[1])

        @pl.when(k == 1)
        def _():
            gather(filler, 0, 2, leg_out.at[1, 0])
            next_rows.start()

            def relay(c):
                leg_rows(c).wait_recv()
                show(2, c).start()

            each(parts, relay)
            gather(wanted[0], 1, 2, leg_out.at[0, 1])
            leg_acc.start()
            gather(filler, 1, 2, leg_out.at[1, 1])
            next_acc.start()
            late_posts(1)

        @pl.when(k == 2)
        def _():
            next_acc.wait_recv()

            def keep(c):
                at = rows_of(c)
                va[3, at] = jnp.where(again, new[2, 1, at], leg_in[1, at])
                for n in range(2):
                    last_out[n, at] = jnp.where(again, leg_in[n, at], new[2, n, at])

            each(parts, keep)
            end_early.start()
            late_posts(2)

        @pl.when(k == 3)
        def _():
            late_posts(3)

    each(BUCKETS * INNER, step)

    for copy in ask + [leg_acc, next_rows, next_acc]:
        copy.wait_send()
    each(4 * parts, lambda q: (show(q // parts, q % parts).wait_send(), share(q // parts, q % parts).wait_send())[0])
    each(parts, lambda c: leg_rows(c).wait_send())
    if final:
        each(halves, lambda h: (bulk(h).wait_send(), bulk(h).wait_recv())[0])
    end_early.wait()
    each(parts, lambda c: (end_late(0, c).wait(), end_late(1, c).wait())[0])

    def unpack(b):
        source = places_s[b]

        def part(c):
            at = rows_of(c)
            items_o[b, at] = inbox[source, 0, at]
            iacc_o[b, at] = inbox[source, 1, at]

        each(parts, part)

    each(blocks, unpack)
    each(INNER, lambda i: store(i).wait())


def put_rows(target, value):
    target[...] = value


def flush_kernel(items, iacc, users, uacc, items_o, iacc_o, users_o, uacc_o, held, sems):
    fetch = pltpu.make_async_copy(uacc, held, sems.at[0])
    fetch.start()
    copies = [
        pltpu.make_async_copy(source, target, sems.at[1 + n])
        for n, (source, target) in enumerate(((users, users_o), (items, items_o), (iacc, iacc_o), (held, uacc_o)))
    ]
    for copy in copies[:3]:
        copy.start()
    fetch.wait()
    copies[3].start()
    for copy in copies:
        copy.wait()


def train_call(first, second, number, plan, operands):
    picks, targets, user_table, user_accum, item_table, item_accum = operands
    rows, width = user_table.shape
    item_rows = item_table.shape[0]
    blocks = item_rows // BLOCK
    span = rows // INNER
    steps = BUCKETS * INNER
    sems = 3 + 11 * 4 + 2 * (blocks - 2) + 4
    f32, bf16 = jnp.float32, jnp.bfloat16
    hbm = pl.BlockSpec(memory_space=pltpu.HBM)
    in_vmem = pl.BlockSpec(memory_space=pltpu.VMEM)
    by_block = (blocks, BLOCK, width)
    pair = (2, BLOCK, width)
    return pl.pallas_call(
        functools.partial(train_kernel, first, second, plan),
        out_shape=(
            jax.ShapeDtypeStruct(by_block, f32),
            jax.ShapeDtypeStruct(by_block, f32),
            jax.ShapeDtypeStruct((rows, width), f32),
            jax.ShapeDtypeStruct((rows, width), f32),
        ),
        in_specs=[pl.BlockSpec(memory_space=pltpu.SMEM)] + [hbm] * 5,
        out_specs=[in_vmem, in_vmem, in_vmem, hbm],
        scratch_shapes=[
            pltpu.VMEM((rows, width), f32),
            pltpu.VMEM((2,) + by_block, f32),
            pltpu.VMEM((BUCKETS, INNER, span), jnp.int32),
            pltpu.VMEM((steps, 1, span), jnp.int32),
            pltpu.VMEM((8, 128), jnp.int32),
            pltpu.VMEM((3, 8, 128), jnp.int32),
            pltpu.SMEM((3, 8, 128), jnp.int32),
            pltpu.SMEM((blocks,), jnp.int32),
            pltpu.SMEM((blocks,), jnp.int32),
            pltpu.SMEM((blocks,), jnp.int32),
            pltpu.VMEM((blocks - 2,) + pair, f32),
            pltpu.VMEM((blocks,) + pair, f32),
            pltpu.VMEM((2,) + pair, f32),
            pltpu.VMEM(pair, f32),
            pltpu.VMEM(pair, f32),
            pltpu.VMEM((steps,) + pair, f32),
            pltpu.VMEM((steps, BLOCK, width), f32),
            pltpu.VMEM((steps,) + pair, f32),
            pltpu.VMEM((steps, BLOCK, width), f32),
            pltpu.VMEM((steps,) + pair, f32),
            pltpu.VMEM((3, span, width), bf16),
            pltpu.VMEM((3, 2 * BLOCK, width), bf16),
            pltpu.VMEM((2 * BLOCK, span), f32),
            pltpu.VMEM((2, 2 * BLOCK, span), bf16),
            pltpu.SemaphoreType.DMA((7,)),
            pltpu.SemaphoreType.DMA((INNER,)),
            pltpu.SemaphoreType.DMA((3,)),
            pltpu.SemaphoreType.DMA((sems,)),
            pltpu.SemaphoreType.DMA((sems,)),
        ],
        compiler_params=pltpu.CompilerParams(
            collective_id=number, has_side_effects=True, vmem_limit_bytes=20 * 1024 * 1024
        ),
        name=f"train_{first}_{second}",
    )(picks, targets, user_table, user_accum, item_table.reshape(by_block), item_accum.reshape(by_block))


def bulk_plan(first, second, count, halves):
    far = count // 2
    if first == second or first == 1:
        plan = (8, 4, 0)
    elif second == 1:
        plan = (6, 6, 0)
    elif first == far and second == 2:
        plan = (4, 2, 3)
    elif far in (first, second):
        plan = (4, 4, 4)
    else:
        plan = (5, 3, 4)
    return plan + (halves - sum(plan),)


def kernel_body(user_table, user_accum, item_table, item_accum, block_pick, positives, partners):
    count = lax.axis_size("dom")
    levels = count.bit_length() - 1
    branches = []
    for a in range(levels):
        for b in range(levels):
            plan = bulk_plan(1 << a, 1 << b, count, 2 * (item_table.shape[0] // BLOCK - 2))
            branches.append(functools.partial(train_branch, 1 << a, 1 << b, a * levels + b, plan))
    masks = partners[:, :1]
    level = sum((masks >> bit & 1) * bit for bit in range(1, levels))
    leading = lax.broadcasted_iota(jnp.int32, level.shape, 0) == 0
    trained = lax.switch(
        jnp.sum(jnp.where(leading, level * levels, level)),
        branches, block_pick, positives, user_table, user_accum, item_table, item_accum,
    )
    hbm, any_space = pl.BlockSpec(memory_space=pltpu.HBM), pl.BlockSpec(memory_space=pl.ANY)
    items, iacc, users, uacc = pl.pallas_call(
        flush_kernel,
        out_shape=tuple(jax.ShapeDtypeStruct(t.shape, t.dtype) for t in trained),
        in_specs=[any_space] * 3 + [hbm],
        out_specs=[hbm] * 4,
        scratch_shapes=[pltpu.VMEM(user_accum.shape, jnp.float32), pltpu.SemaphoreType.DMA((5,))],
        compiler_params=pltpu.CompilerParams(vmem_limit_bytes=2 * 1024 * 1024),
        name="flush",
    )(*trained)
    return users, uacc, items.reshape(item_table.shape), iacc.reshape(item_table.shape)


def train_branch(first, second, number, plan, *operands):
    return train_call(first, second, number, plan, operands)


def trade(block, mask):
    if mask == 0:
        return block
    return lax.ppermute(block, "dom", [(d, d ^ mask) for d in range(lax.axis_size("dom"))])


def train(user_rows, user_acc, chosen, chosen_acc, targets):
    gathered = lax.all_gather(chosen, "grp", axis=0, tiled=True)
    scores = jnp.einsum("ud,bd->ub", user_rows, gathered, precision=HIGHEST)
    onehot = (targets[:, None] == jnp.arange(gathered.shape[0], dtype=jnp.int32)[None, :]).astype(jnp.float32)
    score_grad = jax.nn.softmax(scores, axis=-1) - onehot
    part = jnp.einsum("ub,ud->bd", score_grad, user_rows, precision=HIGH)
    grad_item = lax.psum_scatter(part, "grp", scatter_dimension=0, tiled=True)
    grad_user = jnp.einsum("ub,bd->ud", score_grad, gathered, precision=HIGH)
    return adagrad(user_rows, user_acc, grad_user) + adagrad(chosen, chosen_acc, grad_item)


def take(table, pick):
    return lax.dynamic_slice_in_dim(table, pick * BLOCK, BLOCK, 0)


def put(table, block, pick):
    return lax.dynamic_update_slice_in_dim(table, block, pick * BLOCK, 0)


def newest(tables, updates, pick):
    found = tuple(take(table, pick) for table in tables)
    for at, blocks in updates:
        found = tuple(jnp.where(pick == at, new, old) for new, old in zip(blocks, found))
    return found


def by_level(operands, level, masks):
    branches = [lambda *arrays, mask=mask: tuple(trade(a, mask) for a in arrays) for mask in masks]
    return lax.switch(level, branches, *operands)


def plain_body(user_table, user_accum, item_table, item_accum, block_pick, positives, partners):
    position = lax.axis_index("dom")
    count = lax.axis_size("dom")
    levels = count.bit_length() - 1
    masks = jnp.bitwise_xor(partners[:, position], position)
    level = sum((masks >> bit & 1) * bit for bit in range(levels))
    singles = [1 << bit for bit in range(levels)]
    picks = block_pick[:, :, 0]
    wanted = by_level((picks,), level[0], singles)[0]
    tables = (item_table, item_accum)
    users = list(jnp.split(user_table, INNER))
    uaccs = list(jnp.split(user_accum, INNER))

    updates = []
    for i in range(INNER):
        pick = picks[0, i]
        rows, acc = newest(tables, updates, pick)
        users[i], uaccs[i], rows, acc = train(users[i], uaccs[i], rows, acc, positives[0, i])
        updates.append((pick, (rows, acc)))
    sent = []
    for i in range(INNER):
        sent += newest(tables, updates, wanted[1, i])
    came = by_level((jnp.concatenate(sent),), level[0], singles)[0]
    came = jnp.split(came, 2 * INNER)
    full = list(tables)
    for at, blocks in updates:
        full = [put(table, block, at) for table, block in zip(full, blocks)]

    updates = []
    for i in range(INNER):
        pick = picks[1, i]
        rows, acc = came[2 * i : 2 * i + 2]
        for at, blocks in updates:
            rows, acc = (jnp.where(pick == at, new, old) for new, old in zip(blocks, (rows, acc)))
        users[i], uaccs[i], rows, acc = train(users[i], uaccs[i], rows, acc, positives[1, i])
        updates.append((pick, (rows, acc)))
    late = jnp.concatenate([part for _, blocks in updates for part in blocks])

    def leave(first, second, table, accum, late, picks):
        return (
            trade(table, first ^ second),
            trade(accum, first ^ second),
            trade(late, second),
            trade(picks, second),
        )

    *bulk, late, last_picks = lax.switch(
        level[0] * levels + level[1],
        [functools.partial(leave, first, second) for first in singles for second in singles],
        *full,
        late,
        picks,
    )
    late = jnp.split(late, 2 * INNER)
    for i in range(INNER):
        bulk = [put(t, b, last_picks[1, i]) for t, b in zip(bulk, late[2 * i : 2 * i + 2])]
    return (jnp.concatenate(users, axis=0), jnp.concatenate(uaccs, axis=0), bulk[0], bulk[1])


def solution(mesh):
    rows = P(("grp", "dom"), None)
    columns = P(None, None, ("grp", "dom"))
    return jax.shard_map(
        kernel_body if mesh.shape["grp"] == 2 else plain_body,
        mesh=mesh,
        in_specs=(rows, rows, rows, rows, columns, columns, P()),
        out_specs=(rows, rows, rows, rows),
        check_vma=False,
    )
```

```python
import functools

import jax
import jax.numpy as jnp
from jax import lax
from jax.experimental import pallas as pl
from jax.experimental.pallas import tpu as pltpu
from jax.sharding import PartitionSpec as P

BLOCK = 128
BUCKETS = 2
INNER = 2


learn_rate = 0.3
epsilon = 1e-06

HIGH = lax.Precision.HIGH
HIGHEST = lax.Precision.HIGHEST


def adagrad(param, accum, grad):
    accum = accum + grad * grad
    return (param - learn_rate * grad / (jnp.sqrt(accum) + epsilon), accum)


def each(count, body):
    lax.fori_loop(0, count, lambda n, carry: (body(n), carry)[1], 0)


def order_of(trained, wanted, keys_s, places_s, order_s):
    count = keys_s.shape[0]

    def key(b):
        found = jnp.where(trained[0] == b, 1, 0)
        found = jnp.where(trained[1] == b, 2, found)
        found = jnp.where(wanted[0] == b, 3, found)
        keys_s[b] = jnp.where(wanted[1] == b, 4, found)

    def place(b):
        own = keys_s[b] * count + b
        places_s[b] = sum(jnp.where(keys_s[o] * count + o < own, 1, 0) for o in range(count))

    def block(s):
        order_s[s] = sum(jnp.where(places_s[b] == s, b, 0) for b in range(1, count))

    each(count, key)
    each(count, place)
    if order_s is not None:
        each(count, block)


def split(value, parts):
    for part in parts:
        cut = value.astype(jnp.bfloat16)
        part[...] = cut
        value = value - cut.astype(jnp.float32)


def product(pairs, dims):
    total = None
    for a, b in pairs:
        term = lax.dot_general(a, b, (dims, ((), ())), preferred_element_type=jnp.float32)
        total = term if total is None else total + term
    return total


def train_kernel(
    first, second, plan,
    picks_s, targets_h, users_h, uacc_h, items_h, iacc_h,
    items_o, iacc_o, users, uacc_o,
    uacc, table, raw, targets, tag, tags_v, tags_s, keys_s, places_s, order_s, outbox, inbox, leg_out, leg_in, last_out,
    vv, va, gg, g_in, new, u3, v3, score, g2,
    load_sem, store_sem, tag_sem, send_sem, recv_sem,
):
    g = lax.axis_index("grp")
    d = lax.axis_index("dom")
    final = first ^ second
    blocks = items_h.shape[0]
    span = users_h.shape[0] // INNER
    batch = 2 * BLOCK
    halves = 2 * (blocks - 2)
    chunk = 32
    parts = BLOCK // chunk

    def at_dom(mask):
        there = d
        for bit in range(8):
            if mask >> bit & 1:
                there = there + (1 - 2 * ((d // (1 << bit)) % 2)) * (1 << bit)
        return {"grp": g, "dom": there}

    across = {"grp": 1 - g, "dom": d}
    hop1, hop2 = at_dom(first), at_dom(second)
    hopf = at_dom(final) if final else None

    def load(source, target, k):
        copy = pltpu.make_async_copy(source, target, load_sem.at[k])
        copy.start()
        return copy

    loads = [
        load(items_h, table.at[0], 0),
        load(iacc_h, table.at[1], 2),
        load(users_h.at[pl.ds(0, span)], users.at[pl.ds(0, span)], 1),
        load(users_h.at[pl.ds(span, span)], users.at[pl.ds(span, span)], 3),
        load(uacc_h.at[pl.ds(0, span)], uacc.at[pl.ds(0, span)], 4),
        load(uacc_h.at[pl.ds(span, span)], uacc.at[pl.ds(span, span)], 5),
        load(targets_h, raw, 6),
    ]

    def remote(source, target, k, where):
        return pltpu.make_async_remote_copy(
            source, target, send_sem.at[k], recv_sem.at[k], device_id=where, device_id_type=pl.DeviceIdType.MESH
        )

    def rows_of(c):
        return pl.ds(pl.multiple_of(c * chunk, chunk), chunk)

    ask = [remote(tag, tags_v.at[0], 0, hop1)]
    if final:
        ask += [remote(tag, tags_v.at[1], 1, hop2), remote(tag, tags_v.at[2], 2, hopf)]

    def show(k, c):
        return remote(vv.at[k, 0, rows_of(c)], vv.at[k, 1, rows_of(c)], 3 + k * parts + c, across)

    def share(k, c):
        return remote(gg.at[k, 0, rows_of(c)], g_in.at[k, rows_of(c)], 3 + (4 + k) * parts + c, across)

    sem = 3 + 8 * parts

    def leg_rows(c):
        return remote(leg_out.at[0, 0, rows_of(c)], vv.at[2, 0, rows_of(c)], sem + c, hop1)

    def end_late(n, c):
        return remote(
            new.at[3, n, rows_of(c)], inbox.at[blocks - 1, n, rows_of(c)], sem + (1 + n) * parts + c, hop2
        )

    sem_bulk = sem + 3 * parts

    def bulk(h):
        return remote(outbox.at[h // 2, h % 2], inbox.at[h // 2, h % 2], sem_bulk + h, hopf)

    sem_leg = sem_bulk + halves
    leg_acc = remote(leg_out.at[0, 1], va.at[2], sem_leg, hop1)
    next_rows = remote(leg_out.at[1, 0], leg_in.at[0], sem_leg + 1, hop1)
    next_acc = remote(leg_out.at[1, 1], leg_in.at[1], sem_leg + 2, hop1)
    end_early = remote(last_out, inbox.at[blocks - 2], sem_leg + 3, hop2)

    mine = [picks_s[k // INNER, k % INNER, 0] for k in range(BUCKETS * INNER)]
    lane = lax.broadcasted_iota(jnp.int32, tag.shape, 1)
    told = jnp.zeros(tag.shape, jnp.int32)
    for k in range(BUCKETS * INNER):
        told = jnp.where(lane == k, mine[k], told)
    tag[...] = told

    barrier = pltpu.get_barrier_semaphore()
    peers = [across, hop1] + ([hop2, hopf] if final else [])
    for where in peers:
        pl.semaphore_signal(barrier, inc=1, device_id=where, device_id_type=pl.DeviceIdType.MESH)
    loads[0].wait()
    loads[1].wait()
    each(parts, lambda c: put_rows(vv.at[0, 0, rows_of(c)], table[0, mine[0], rows_of(c)]))
    pl.semaphore_wait(barrier, len(peers))
    for copy in ask:
        copy.start()
    each(parts, lambda c: show(0, c).start())
    again = mine[2] == mine[3]

    each(parts, lambda c: put_rows(va.at[0, rows_of(c)], table[1, mine[0], rows_of(c)]))

    def hear(n):
        ask[n].wait_recv()
        copy = pltpu.make_async_copy(tags_v.at[n], tags_s.at[n], tag_sem.at[n])
        copy.start()
        copy.wait()

    hear(0)
    wanted = [tags_s[0, 0, 2], tags_s[0, 0, 3]]
    order_of(mine[:2], wanted, keys_s, places_s, order_s)
    filler = jnp.where(wanted[0] == wanted[1], order_s[blocks - 2], wanted[1])
    def newest(pick, n, at, upto):
        value = table[n, pick, at]
        for k in range(upto):
            value = jnp.where(mine[k] == pick, new[k, n, at], value)
        return value

    def gather(pick, n, upto, target):
        each(parts, lambda c: put_rows(target.at[rows_of(c)], newest(pick, n, rows_of(c), upto)))

    def post(h, upto):
        box = outbox if final else inbox
        gather(order_s[h // 2], h % 2, upto, box.at[h // 2, h % 2])
        if final:
            bulk(h).start()

    each(plan[0], lambda h: post(h, 0))
    if final:
        hear(1)
        hear(2)
        order_of([tags_s[2, 0, 0], tags_s[2, 0, 1]], [tags_s[1, 0, 2], tags_s[1, 0, 3]], keys_s, places_s, None)

    def late_posts(group):
        if plan[group]:
            each(plan[group], lambda h: post(h + sum(plan[:group]), 2))

    loads[6].wait()
    for k in range(BUCKETS * INNER):
        targets[k] = raw[k // INNER, pl.ds(k % INNER, 1)]
    row = lax.broadcasted_iota(jnp.int32, (batch, BLOCK), 0)
    nt, nn, tn = ((1,), (1,)), ((1,), (0,)), ((0,), (0,))

    def store(i):
        rows_u = pl.ds(pl.multiple_of(i * span, span), span)
        return pltpu.make_async_copy(uacc.at[rows_u], uacc_o.at[rows_u], store_sem.at[i])

    def step(k):
        base = (k % INNER) * span
        for i in range(INNER):
            @pl.when(k == i)
            def _():
                loads[2 + i].wait()

        def split_users(t):
            at = pl.ds(pl.multiple_of(t * BLOCK, BLOCK), BLOCK)
            split(users[pl.ds(pl.multiple_of(base + t * BLOCK, BLOCK), BLOCK)], [u3.at[n, at] for n in range(3)])

        each(span // BLOCK, split_users)

        def score_half(h):
            def split_items(c):
                @pl.when(h == 1)
                def _():
                    show(k, c).wait_recv()

                at = pl.ds(pl.multiple_of(h * BLOCK + c * chunk, chunk), chunk)
                split(vv[k, h, rows_of(c)], [v3.at[n, at] for n in range(3)])

            each(parts, split_items)
            at = pl.ds(pl.multiple_of(h * BLOCK, BLOCK), BLOCK)

            def tile(t):
                cols = pl.ds(pl.multiple_of(t * batch, batch), batch)
                v = [v3[n, at] for n in range(3)]
                u = [u3[n, cols] for n in range(3)]
                score[at, cols] = product(
                    [(v[2], u[0]), (v[0], u[2]), (v[1], u[1]), (v[1], u[0]), (v[0], u[1]), (v[0], u[0])], nt
                )

            each(span // batch, tile)

        each(2, score_half)

        def soften(t):
            cols = pl.ds(pl.multiple_of(t * BLOCK, BLOCK), BLOCK)
            s = score[:, cols]
            e = jnp.exp(s - jnp.max(s, 0, keepdims=True))
            target = (targets[k, :, cols] - g * BLOCK) & (batch - 1)
            grad = e * (1.0 / jnp.sum(e, 0, keepdims=True)) - jnp.where(row == target, 1.0, 0.0)
            split(grad, [g2.at[n, :, cols] for n in range(2)])

        each(span // BLOCK, soften)

        def item_part(h):
            at = pl.ds(pl.multiple_of((1 - h) * BLOCK, BLOCK), BLOCK)
            hi, lo = g2[0, at], g2[1, at]
            gg[k, h] = product([(lo, u3[0]), (hi, u3[1]), (hi, u3[0])], nn)

            @pl.when(h == 0)
            def _():
                each(parts, lambda c: share(k, c).start())

        each(2, item_part)
        for i in range(INNER):
            @pl.when(k == i)
            def _():
                loads[4 + i].wait()

        def user_part(t):
            cols = pl.ds(pl.multiple_of(t * BLOCK, BLOCK), BLOCK)
            at = pl.ds(pl.multiple_of(base + t * BLOCK, BLOCK), BLOCK)
            hi, lo = g2[0, :, cols], g2[1, :, cols]
            grad = product([(lo, v3[0]), (hi, v3[1]), (hi, v3[0])], tn)
            users[at], uacc[at] = adagrad(users[at], uacc[at], grad)

        each(span // BLOCK, user_part)

        @pl.when(k >= INNER)
        def _():
            store(k % INNER).start()

        @pl.when(k == 2)
        def _():
            next_rows.wait_recv()
            leg_acc.wait_recv()

        def item_rows(c):
            at = rows_of(c)
            share(k, c).wait_recv()
            new[k, 0, at], new[k, 1, at] = adagrad(vv[k, 0, at], va[k, at], gg[k, 1, at] + g_in[k, at])

            @pl.when(k == 0)
            def _():
                vv[1, 0, at] = newest(mine[1], 0, at, 1)
                show(1, c).start()

            @pl.when(k == 1)
            def _():
                leg_out[0, 0, at] = newest(wanted[0], 0, at, 2)
                leg_rows(c).start()

            @pl.when(k == 2)
            def _():
                vv[3, 0, at] = jnp.where(again, new[2, 0, at], leg_in[0, at])
                show(3, c).start()

            @pl.when(k == 3)
            def _():
                end_late(0, c).start()
                end_late(1, c).start()

        each(parts, item_rows)

        @pl.when(k == 0)
        def _():
            gather(mine[1], 1, 1, va.at[1])

        @pl.when(k == 1)
        def _():
            gather(filler, 0, 2, leg_out.at[1, 0])
            next_rows.start()

            def relay(c):
                leg_rows(c).wait_recv()
                show(2, c).start()

            each(parts, relay)
            gather(wanted[0], 1, 2, leg_out.at[0, 1])
            leg_acc.start()
            gather(filler, 1, 2, leg_out.at[1, 1])
            next_acc.start()
            late_posts(1)

        @pl.when(k == 2)
        def _():
            next_acc.wait_recv()

            def keep(c):
                at = rows_of(c)
                va[3, at] = jnp.where(again, new[2, 1, at], leg_in[1, at])
                for n in range(2):
                    last_out[n, at] = jnp.where(again, leg_in[n, at], new[2, n, at])

            each(parts, keep)
            end_early.start()
            late_posts(2)

        @pl.when(k == 3)
        def _():
            late_posts(3)

    each(BUCKETS * INNER, step)

    for copy in ask + [leg_acc, next_rows, next_acc]:
        copy.wait_send()
    each(4 * parts, lambda q: (show(q // parts, q % parts).wait_send(), share(q // parts, q % parts).wait_send())[0])
    each(parts, lambda c: leg_rows(c).wait_send())
    if final:
        each(halves, lambda h: (bulk(h).wait_send(), bulk(h).wait_recv())[0])
    end_early.wait()
    each(parts, lambda c: (end_late(0, c).wait(), end_late(1, c).wait())[0])

    def unpack(b):
        source = places_s[b]

        def part(c):
            at = rows_of(c)
            items_o[b, at] = inbox[source, 0, at]
            iacc_o[b, at] = inbox[source, 1, at]

        each(parts, part)

    each(blocks, unpack)
    each(INNER, lambda i: store(i).wait())


def put_rows(target, value):
    target[...] = value


def flush_kernel(items, iacc, users, uacc, items_o, iacc_o, users_o, uacc_o, held, sems):
    fetch = pltpu.make_async_copy(uacc, held, sems.at[0])
    fetch.start()
    copies = [
        pltpu.make_async_copy(source, target, sems.at[1 + n])
        for n, (source, target) in enumerate(((users, users_o), (items, items_o), (iacc, iacc_o), (held, uacc_o)))
    ]
    for copy in copies[:3]:
        copy.start()
    fetch.wait()
    copies[3].start()
    for copy in copies:
        copy.wait()


def train_call(first, second, number, plan, operands):
    picks, targets, user_table, user_accum, item_table, item_accum = operands
    rows, width = user_table.shape
    item_rows = item_table.shape[0]
    blocks = item_rows // BLOCK
    span = rows // INNER
    steps = BUCKETS * INNER
    sems = 3 + 11 * 4 + 2 * (blocks - 2) + 4
    f32, bf16 = jnp.float32, jnp.bfloat16
    hbm = pl.BlockSpec(memory_space=pltpu.HBM)
    in_vmem = pl.BlockSpec(memory_space=pltpu.VMEM)
    by_block = (blocks, BLOCK, width)
    pair = (2, BLOCK, width)
    return pl.pallas_call(
        functools.partial(train_kernel, first, second, plan),
        out_shape=(
            jax.ShapeDtypeStruct(by_block, f32),
            jax.ShapeDtypeStruct(by_block, f32),
            jax.ShapeDtypeStruct((rows, width), f32),
            jax.ShapeDtypeStruct((rows, width), f32),
        ),
        in_specs=[pl.BlockSpec(memory_space=pltpu.SMEM)] + [hbm] * 5,
        out_specs=[in_vmem, in_vmem, in_vmem, hbm],
        scratch_shapes=[
            pltpu.VMEM((rows, width), f32),
            pltpu.VMEM((2,) + by_block, f32),
            pltpu.VMEM((BUCKETS, INNER, span), jnp.int32),
            pltpu.VMEM((steps, 1, span), jnp.int32),
            pltpu.VMEM((8, 128), jnp.int32),
            pltpu.VMEM((3, 8, 128), jnp.int32),
            pltpu.SMEM((3, 8, 128), jnp.int32),
            pltpu.SMEM((blocks,), jnp.int32),
            pltpu.SMEM((blocks,), jnp.int32),
            pltpu.SMEM((blocks,), jnp.int32),
            pltpu.VMEM((blocks - 2,) + pair, f32),
            pltpu.VMEM((blocks,) + pair, f32),
            pltpu.VMEM((2,) + pair, f32),
            pltpu.VMEM(pair, f32),
            pltpu.VMEM(pair, f32),
            pltpu.VMEM((steps,) + pair, f32),
            pltpu.VMEM((steps, BLOCK, width), f32),
            pltpu.VMEM((steps,) + pair, f32),
            pltpu.VMEM((steps, BLOCK, width), f32),
            pltpu.VMEM((steps,) + pair, f32),
            pltpu.VMEM((3, span, width), bf16),
            pltpu.VMEM((3, 2 * BLOCK, width), bf16),
            pltpu.VMEM((2 * BLOCK, span), f32),
            pltpu.VMEM((2, 2 * BLOCK, span), bf16),
            pltpu.SemaphoreType.DMA((7,)),
            pltpu.SemaphoreType.DMA((INNER,)),
            pltpu.SemaphoreType.DMA((3,)),
            pltpu.SemaphoreType.DMA((sems,)),
            pltpu.SemaphoreType.DMA((sems,)),
        ],
        compiler_params=pltpu.CompilerParams(
            collective_id=number, has_side_effects=True, vmem_limit_bytes=20 * 1024 * 1024
        ),
        name=f"train_{first}_{second}",
    )(picks, targets, user_table, user_accum, item_table.reshape(by_block), item_accum.reshape(by_block))


def bulk_plan(first, second, count, halves):
    far = count // 2
    if first == second or first == 1:
        plan = (8, 4, 0)
    elif second == 1:
        plan = (6, 6, 0)
    elif first == far and second == 2:
        plan = (4, 2, 3)
    elif far in (first, second):
        plan = (4, 4, 4)
    else:
        plan = (5, 3, 4)
    return plan + (halves - sum(plan),)


def kernel_body(user_table, user_accum, item_table, item_accum, block_pick, positives, partners):
    count = lax.axis_size("dom")
    levels = count.bit_length() - 1
    branches = []
    for a in range(levels):
        for b in range(levels):
            plan = bulk_plan(1 << a, 1 << b, count, 2 * (item_table.shape[0] // BLOCK - 2))
            branches.append(functools.partial(train_branch, 1 << a, 1 << b, a * levels + b, plan))
    masks = partners[:, :1]
    level = sum((masks >> bit & 1) * bit for bit in range(1, levels))
    leading = lax.broadcasted_iota(jnp.int32, level.shape, 0) == 0
    trained = lax.switch(
        jnp.sum(jnp.where(leading, level * levels, level)),
        branches, block_pick, positives, user_table, user_accum, item_table, item_accum,
    )
    hbm, any_space = pl.BlockSpec(memory_space=pltpu.HBM), pl.BlockSpec(memory_space=pl.ANY)
    items, iacc, users, uacc = pl.pallas_call(
        flush_kernel,
        out_shape=tuple(jax.ShapeDtypeStruct(t.shape, t.dtype) for t in trained),
        in_specs=[any_space] * 3 + [hbm],
        out_specs=[hbm] * 4,
        scratch_shapes=[pltpu.VMEM(user_accum.shape, jnp.float32), pltpu.SemaphoreType.DMA((5,))],
        compiler_params=pltpu.CompilerParams(vmem_limit_bytes=2 * 1024 * 1024),
        name="flush",
    )(*trained)
    return users, uacc, items.reshape(item_table.shape), iacc.reshape(item_table.shape)


def train_branch(first, second, number, plan, *operands):
    return train_call(first, second, number, plan, operands)


def trade(block, mask):
    if mask == 0:
        return block
    return lax.ppermute(block, "dom", [(d, d ^ mask) for d in range(lax.axis_size("dom"))])


def train(user_rows, user_acc, chosen, chosen_acc, targets):
    gathered = lax.all_gather(chosen, "grp", axis=0, tiled=True)
    scores = jnp.einsum("ud,bd->ub", user_rows, gathered, precision=HIGHEST)
    onehot = (targets[:, None] == jnp.arange(gathered.shape[0], dtype=jnp.int32)[None, :]).astype(jnp.float32)
    score_grad = jax.nn.softmax(scores, axis=-1) - onehot
    part = jnp.einsum("ub,ud->bd", score_grad, user_rows, precision=HIGH)
    grad_item = lax.psum_scatter(part, "grp", scatter_dimension=0, tiled=True)
    grad_user = jnp.einsum("ub,bd->ud", score_grad, gathered, precision=HIGH)
    return adagrad(user_rows, user_acc, grad_user) + adagrad(chosen, chosen_acc, grad_item)


def take(table, pick):
    return lax.dynamic_slice_in_dim(table, pick * BLOCK, BLOCK, 0)


def put(table, block, pick):
    return lax.dynamic_update_slice_in_dim(table, block, pick * BLOCK, 0)


def newest(tables, updates, pick):
    found = tuple(take(table, pick) for table in tables)
    for at, blocks in updates:
        found = tuple(jnp.where(pick == at, new, old) for new, old in zip(blocks, found))
    return found


def by_level(operands, level, masks):
    branches = [lambda *arrays, mask=mask: tuple(trade(a, mask) for a in arrays) for mask in masks]
    return lax.switch(level, branches, *operands)


def plain_body(user_table, user_accum, item_table, item_accum, block_pick, positives, partners):
    position = lax.axis_index("dom")
    count = lax.axis_size("dom")
    levels = count.bit_length() - 1
    masks = jnp.bitwise_xor(partners[:, position], position)
    level = sum((masks >> bit & 1) * bit for bit in range(levels))
    singles = [1 << bit for bit in range(levels)]
    picks = block_pick[:, :, 0]
    wanted = by_level((picks,), level[0], singles)[0]
    tables = (item_table, item_accum)
    users = list(jnp.split(user_table, INNER))
    uaccs = list(jnp.split(user_accum, INNER))

    updates = []
    for i in range(INNER):
        pick = picks[0, i]
        rows, acc = newest(tables, updates, pick)
        users[i], uaccs[i], rows, acc = train(users[i], uaccs[i], rows, acc, positives[0, i])
        updates.append((pick, (rows, acc)))
    sent = []
    for i in range(INNER):
        sent += newest(tables, updates, wanted[1, i])
    came = by_level((jnp.concatenate(sent),), level[0], singles)[0]
    came = jnp.split(came, 2 * INNER)
    full = list(tables)
    for at, blocks in updates:
        full = [put(table, block, at) for table, block in zip(full, blocks)]

    updates = []
    for i in range(INNER):
        pick = picks[1, i]
        rows, acc = came[2 * i : 2 * i + 2]
        for at, blocks in updates:
            rows, acc = (jnp.where(pick == at, new, old) for new, old in zip(blocks, (rows, acc)))
        users[i], uaccs[i], rows, acc = train(users[i], uaccs[i], rows, acc, positives[1, i])
        updates.append((pick, (rows, acc)))
    late = jnp.concatenate([part for _, blocks in updates for part in blocks])

    def leave(first, second, table, accum, late, picks):
        return (
            trade(table, first ^ second),
            trade(accum, first ^ second),
            trade(late, second),
            trade(picks, second),
        )

    *bulk, late, last_picks = lax.switch(
        level[0] * levels + level[1],
        [functools.partial(leave, first, second) for first in singles for second in singles],
        *full,
        late,
        picks,
    )
    late = jnp.split(late, 2 * INNER)
    for i in range(INNER):
        bulk = [put(t, b, last_picks[1, i]) for t, b in zip(bulk, late[2 * i : 2 * i + 2])]
    return (jnp.concatenate(users, axis=0), jnp.concatenate(uaccs, axis=0), bulk[0], bulk[1])


def solution(mesh):
    rows = P(("grp", "dom"), None)
    columns = P(None, None, ("grp", "dom"))
    return jax.shard_map(
        kernel_body if mesh.shape["grp"] == 2 else plain_body,
        mesh=mesh,
        in_specs=(rows, rows, rows, rows, columns, columns, P()),
        out_specs=(rows, rows, rows, rows),
        check_vma=False,
    )
```
